32 devices in a mesh: outer: 4 (over z), inner: 8 (over y, x, core).
Axes of the slice: x: 2, y: 2, z: 4, core: 2. Of those that a mesh axis runs over, the one named last changes fastest.
Arguments:
- g_emb: float32 [32, 4096, 768], P(('outer', 'inner'))
- g_qkv: float32 [32, 1, 768, 2304], P(('outer', 'inner'))
- g_o: float32 [32, 1, 768, 768], P(('outer', 'inner'))
- g_w1: float32 [32, 1, 768, 2048], P(('outer', 'inner'))
- g_w2: float32 [32, 1, 2048, 768], P(('outer', 'inner'))
- g_bqkv: float32 [32, 1, 2304], P(('outer', 'inner'))
- g_b1: float32 [32, 1, 2048], P(('outer', 'inner'))
- g_dvec: float32 [32, 1, 6, 768], P(('outer', 'inner'))
- m: float32 [8659712], P(('outer', 'inner'))
- v: float32 [8659712], P(('outer', 'inner'))
- w: float32 [8659712], P(('outer', 'inner'))
- lr: float32 [], replicated
- beta1: float32 [], replicated
- beta2: float32 [], replicated
- eps: float32 [], replicated
- step: int32 [], replicated
Outputs:
- output 1: float32 [8659712], P(('outer', 'inner'))
- output 2: float32 [8659712], P(('outer', 'inner'))
- output 3: float32 [8659712], P(('outer', 'inner'))
- output 4: bfloat16 [4096, 768], replicated
- output 5: bfloat16 [1, 768, 2304], replicated
- output 6: bfloat16 [1, 768, 768], replicated
- output 7: bfloat16 [1, 768, 2048], replicated
- output 8: bfloat16 [1, 2048, 768], replicated
- output 9: bfloat16 [1, 2304], replicated
- output 10: bfloat16 [1, 2048], replicated
- output 11: bfloat16 [1, 6, 768], replicated
All inputs are finite; a program needn't handle non-finite values.
Results may differ from the reference program's by a relative error of at most 0.001.
Values are sent between devices in bfloat16 or wider.
A program may use at most 1 GiB of HBM per device.

```python
import math
import jax
import jax.numpy as jnp

DEVICES = 32
D = 768
FF = 2048
LAYERS = 1
EMB_ROWS = 4096

SHAPES = (
    (EMB_ROWS, D),
    (LAYERS, D, 3 * D),
    (LAYERS, D, D),
    (LAYERS, D, FF),
    (LAYERS, FF, D),
    (LAYERS, 3 * D),
    (LAYERS, FF),
    (LAYERS, 6, D),
)
SIZES = tuple(math.prod(s) for s in SHAPES)
PSI = sum(SIZES)
NAMES = ("g_emb", "g_qkv", "g_o", "g_w1", "g_w2", "g_bqkv", "g_b1", "g_dvec")


def draw_grad(key, shape):
    k1, k2 = jax.random.split(key)
    common = jax.random.normal(k1, shape, jnp.float32)
    own = jax.random.normal(k2, (DEVICES,) + shape, jnp.float32)
    return common[None] + 4.0 * own


def setup_inputs(seed: int = 0) -> dict:
    ks = jax.random.split(jax.random.key(seed), 16)
    out = {}
    for i in range(8):
        out[NAMES[i]] = draw_grad(ks[i], SHAPES[i])
    out["m"] = jax.random.normal(ks[8], (PSI,), jnp.float32)
    out["v"] = jax.random.uniform(ks[9], (PSI,), jnp.float32, 1.0, 4.0)
    out["w"] = jax.random.normal(ks[10], (PSI,), jnp.float32)
    out["lr"] = jax.random.uniform(ks[11], (), jnp.float32, 0.12, 0.2)
    out["beta1"] = jax.random.uniform(ks[12], (), jnp.float32, 0.5, 0.7)
    out["beta2"] = jax.random.uniform(ks[13], (), jnp.float32, 0.7, 0.9)
    out["eps"] = jax.random.uniform(ks[14], (), jnp.float32, 0.1, 1.5)
    out["step"] = jax.random.randint(ks[15], (), 1, 6, jnp.int32)
    return out


def reference(g_emb, g_qkv, g_o, g_w1, g_w2, g_bqkv, g_b1, g_dvec, m, v, w, lr, beta1, beta2, eps, step):
    grads = (g_emb, g_qkv, g_o, g_w1, g_w2, g_bqkv, g_b1, g_dvec)
    g = jnp.concatenate([jnp.sum(x, axis=0).reshape(-1) for x in grads]) / DEVICES
    t = step.astype(jnp.float32)
    m_new = beta1 * m + (1.0 - beta1) * g
    v_new = beta2 * v + (1.0 - beta2) * (g * g)
    m_hat = m_new / (1.0 - beta1 ** t)
    v_hat = v_new / (1.0 - beta2 ** t)
    w_new = w - lr * m_hat / (jnp.sqrt(v_hat) + eps)
    flat = w_new.astype(jnp.bfloat16)
    wb = []
    start = 0
    for i in range(8):
        wb.append(flat[start:start + SIZES[i]].reshape(SHAPES[i]))
        start = start + SIZES[i]
    return (m_new, v_new, w_new, wb[0], wb[1], wb[2], wb[3], wb[4], wb[5], wb[6], wb[7])
```

```python
import functools
import math

import jax
import jax.numpy as jnp
from jax import lax
from jax.experimental import pallas as pl
from jax.experimental.pallas import tpu as pltpu
from jax.sharding import PartitionSpec as P

AXES = ("outer", "inner")
MESH = pl.DeviceIdType.MESH
F32 = jnp.float32
BF16 = jnp.bfloat16

DEV = 32
SHARD = 270616
ROWS16 = 33827
TENSORS = ((0, 24576, 6), (24576, 38400, 18), (38400, 43008, 6), (43008, 55296, 16), (55296, 67584, 6))
TAIL0 = 67584
TAIL_ROWS = 80
LAST_ROW = 67654
NR = 2128
K = 19
NA, NB, NC = 40, 48, 24
CH = NA + NB + NC
SL = 4
S0 = 5
AHEAD = 2
HALO = 160
LOCPAD = 24
LROWS = 2120
FROWS = 2464


def win_start(r):
    if isinstance(r, int):
        return (r * ROWS16) // 256 * 16
    return lax.div(r * ROWS16, 256) * 16


def rows_of(r):
    lo, hi = win_start(r), win_start(r) + NR
    segs = []
    for i, (a, b, _) in enumerate(TENSORS + ((TAIL0, TAIL0 + TAIL_ROWS, 1),)):
        s, e = max(lo, a), min(hi, b)
        if s < e:
            segs.append((i, s - a, s - lo, e - s))
    return segs


def al(i, n, a=8):
    return pl.ds(pl.multiple_of(i, a), n)


def bits(w, n):
    out = []
    for _ in range(n):
        out.append(lax.rem(w, 2))
        w = lax.div(w, 2)
    return tuple(out[::-1])


def loop_add(dst, src, lead, n):
    def one(w, _):
        d, s = dst(w), src(w)
        for o in range(0, n, 8):
            d[pl.ds(o, 8), :] = d[pl.ds(o, 8), :] + s[pl.ds(o, 8), :]
        return 0

    lax.fori_loop(0, lead, one, 0)


def adam(g, m, v, w, sc):
    lr, b1, c1, b2, c2, i1, i2, eps = sc
    m2 = b1 * m + c1 * g
    v2 = b2 * v + c2 * (g * g)
    w2 = w - lr * (m2 * i1) / (jnp.sqrt(v2 * i2) + eps)
    return m2, v2, w2


H, L, Y, X = range(4)
ORDERS = ((X, Y, L, H), (Y, X, L, H), (L, H, X, Y))
PARTS = (NA, NB, NC)
STARTS = (0, NA, NA + NB)
NST = len(ORDERS[0])


def comm_kernel(sc_ref, e_ref, q_ref, o_ref, w1_ref, w2_ref, t_ref, m_ref, v_ref, w_ref, ag, out3, *scratch):
    bufs, scratch = scratch[:3 * NST], scratch[3 * NST:]
    (S, R0, LOC, F, TIL, HP, HN, GT, GP, GN, FG, WB,
     ld, s0s, s0r, rss, rsr, ags, agr, fws, fwr, lcl, mvs, hs, hr, osem) = scratch
    z = lax.axis_index(AXES[0])
    inner = lax.axis_index(AXES[1])
    h, l, y, x, c = bits(z, 2) + bits(inner, 3)
    me = (h, l, y, x)
    r = z * 8 + inner
    g_refs = (e_ref, q_ref, o_ref, w1_ref, w2_ref, t_ref)
    sc = [sc_ref[i] for i in range(8)]

    def flip(ax):
        p = [1 - b if i == ax else b for i, b in enumerate(me)]
        return p[H] * 2 + p[L], p[Y] * 4 + p[X] * 2 + c

    PEER = [flip(ax) for ax in range(4)]
    CORE = (z, inner + 1 - 2 * c)

    def device(i):
        i = lax.rem(i, DEV)
        return lax.div(i, 8), lax.rem(i, 8)

    NXT, PRV = device(r + 1), device(r + DEV - 1)

    def remote(src, dst, ss, rs, dev):
        return pltpu.make_async_remote_copy(src_ref=src, dst_ref=dst, send_sem=ss, recv_sem=rs,
                                            device_id=dev, device_id_type=MESH)

    def window_copies(w, q, make):
        segs = rows_of(w)
        off = q * CH
        if len(segs) == 1:
            i, a, _, _ = segs[0]
            make(g_refs[i].at[al(a + off, CH)], 0, CH)
            return
        for n, (i, a, b, size) in enumerate(segs):
            first, last = -(-b // CH), (b + size) // CH

            @pl.when(jnp.logical_and(q >= first, q < last))
            def _(i=i, a=a, b=b):
                make(g_refs[i].at[al(jnp.maximum(a + off - b, 0), CH)], 0, CH)

            if n + 1 < len(segs) and (b + size) % CH:
                edge, head = (b + size) // CH, (b + size) % CH
                j, a2, _, _ = segs[n + 1]

                @pl.when(q == edge)
                def _(i=i, a=a, size=size, head=head, j=j, a2=a2):
                    make(g_refs[i].at[pl.ds(a + size - head, head)], 0, head)
                    make(g_refs[j].at[pl.ds(a2, CH - head)], head, CH - head)

    def start0(q):
        slot = lax.rem(q, S0)
        for par in range(2):

            @pl.when(c == par)
            def _(par=par):
                for k in range(16):
                    idx = tuple(k >> i & 1 for i in (3, 2, 1, 0))

                    def send(src, o, n, idx=idx):
                        remote(src, R0.at[(slot,) + idx + (pl.ds(o, n),)], s0s.at[slot], s0r.at[slot], CORE).start()

                    def load(src, o, n, idx=idx):
                        pltpu.make_async_copy(src, S.at[idx + (al(q * CH + o, n),)], ld.at[slot]).start()

                    window_copies(2 * k + 1 - par, q, send)
                    window_copies(2 * k + par, q, load)

    def wait0(q):
        slot = lax.rem(q, S0)
        rows = S.at[:, :, :, :, al(q * CH, CH)]
        pltpu.make_async_copy(rows, rows, ld.at[slot]).wait()
        remote(R0.at[slot], R0.at[slot], s0s.at[slot], s0r.at[slot], CORE).wait()

    every = slice(None)

    def part(k, q):
        return al(q * CH + STARTS[k], PARTS[k])

    def where_rs(k, st, q, other):
        o = ORDERS[k]
        idx = [every] * 4
        for ax in o[:st]:
            idx[ax] = me[ax]
        idx[o[st]] = 1 - me[o[st]] if other else me[o[st]]
        return idx + [part(k, q)]

    def where_ag(k, st, q, other, core):
        o = ORDERS[k][::-1]
        idx = list(me)
        for ax in o[:st]:
            idx[ax] = every
        idx[o[st]] = 1 - me[o[st]] if other else me[o[st]]
        return tuple(idx + [core, part(k, q)])

    def rs_copy(k, st, q):
        s = lax.rem(q, SL)
        return remote(S.at[tuple(where_rs(k, st, q, True))], bufs[k * NST + st].at[s],
                      rss.at[k, st, s], rsr.at[k, st, s], PEER[ORDERS[k][st]])

    def ag_copy(k, st, q, recv):
        s = lax.rem(q, SL)
        dst = ag.at[where_ag(k, st, q, recv, c)]
        src = WB.at[part(k, q)] if st == 0 else dst
        return remote(src, dst, ags.at[k, st, s], agr.at[k, st, s], PEER[ORDERS[k][NST - 1 - st]])

    def fw_copy(k, st, q, core):
        s = lax.rem(q, SL)
        idx = list(where_ag(k, st, q, True, core))
        if st == 0:
            idx[ORDERS[k][NST - 1]] = every
        ref = ag.at[tuple(idx)]
        return remote(ref, ref, fws.at[k, st, s], fwr.at[k, st, s], CORE)

    def start(cp, q):
        @pl.when(q >= SL)
        def _():
            cp.wait_send()

        cp.start()

    def own_copy(q):
        return pltpu.make_async_copy(WB.at[al(q * CH, CH)], ag.at[me + (c, al(q * CH, CH))], lcl.at[lax.rem(q, SL)])

    def reduce_stage(k, st, q):
        rs_copy(k, st, q).wait_recv()
        s = lax.rem(q, SL)
        idx = where_rs(k, st, q, False)
        free = ORDERS[k][st + 1:]

        def dst(w):
            at = list(idx)
            for ax, b in zip(sorted(free), bits(w, len(free))):
                at[ax] = b
            return S.at[tuple(at)]

        loop_add(dst, lambda w: bufs[k * NST + st].at[(s,) + bits(w, len(free))], 2 ** len(free), PARTS[k])

    sr, srn = win_start(r), win_start(r + 1)
    delta = lax.rem(r * 24, 128)
    drow = lax.div(r * ROWS16, 16) - sr
    edge_n = lax.rem((r + 1) * 24, 128) + 128 * (lax.div((r + 1) * ROWS16, 16) - srn)
    nb = HALO + srn - sr
    lane = lax.broadcasted_iota(jnp.int32, (8, 128), 1)
    sub = lax.broadcasted_iota(jnp.int32, (8, 128), 0)

    def halo_copies():
        return [remote(F.at[:, al(nb - HALO, HALO + 16)], HP, hs.at[0], hr.at[0], NXT),
                remote(F.at[:, pl.ds(HALO, HALO + 16)], HN, hs.at[1], hr.at[1], PRV)]

    def state_copies():
        return [pltpu.make_async_copy(ref, LOC.at[k, pl.ds(LOCPAD, LROWS)], mvs.at[k])
                for k, ref in enumerate((m_ref, v_ref, w_ref))]

    def shift(ref, at, other, by, keep):
        a = pltpu.roll(ref[pl.ds(at, 8), :], by, 1)
        b = pltpu.roll(ref[pl.ds(at + other, 8), :], by, 1)
        return jnp.where(keep, a, b)

    def prepare1():
        for cp in state_copies():
            cp.wait()
        keep = lane >= delta

        def one(i, _):
            for j in range(4):
                at = i * 32 + j * 8
                for k in range(3):
                    F[k, al(HALO + at, 8), :] = shift(LOC.at[k], LOCPAD + at - drow, -1, delta, keep)
            return 0

        lax.fori_loop(0, (NR + 16) // 32, one, 0)
        for cp in halo_copies():
            cp.start()

    def blocks(first, last, body):
        for a, b, wt in TENSORS + ((TAIL0, TAIL0 + TAIL_ROWS, 1),):
            lo = lax.div(jnp.maximum(first - a, 0), 8 * wt)
            hi = lax.div(jnp.maximum(jnp.minimum(last, b) - a, 0) + 8 * wt - 1, 8 * wt)

            def one(i, _, a=a, wt=wt):
                body(a + i * 8 * wt, wt)
                return 0

            lax.fori_loop(lo, hi, one, 0)

    def prepare2():
        for cp in halo_copies():
            cp.wait()
        for k in range(3):
            for i in range(0, 16, 8):
                idx = (sub + i) * 128 + lane
                o = pl.ds(HALO + i, 8)
                F[k, o, :] = jnp.where(idx < drow * 128 + delta, HP[k, o, :], F[k, o, :])
                o = al(nb + i, 8)
                F[k, o, :] = jnp.where(idx >= edge_n, HN[k, pl.ds(i, 8), :], F[k, o, :])

        def one(i, _):
            for k in range(3):
                F[k, al(i * 16, 16), :] = HP[k, al(i * 16, 16), :]
                F[k, al(nb + 16 + i * 16, 16), :] = HN[k, al(16 + i * 16, 16), :]
            return 0

        lax.fori_loop(0, HALO // 16, one, 0)

        def permute(row, wt):
            at = row - sr + HALO
            for j in range(wt):
                for k in range(3):
                    TIL[k, al(at + 8 * j, 8), :] = (
                        F[k, pl.ds(at + j, 8, stride=wt), :] if wt > 1 else F[k, al(at, 8), :])

        blocks(sr, sr + NR, permute)

    def ghalo_copies():
        return [remote(GT.at[al(nb - HALO, HALO)], GP, hs.at[2], hr.at[2], NXT),
                remote(GT.at[pl.ds(HALO, HALO + 16)], GN, hs.at[3], hr.at[3], PRV)]

    def finish1():
        for cp in ghalo_copies():
            cp.start()

    def finish2():
        for cp in ghalo_copies():
            cp.wait()

        def put(i, _):
            GT[al(i * 16, 16), :] = GP[al(i * 16, 16), :]
            GT[al(HALO + NR + i * 16, 16), :] = GN[al(HALO + NR - nb + i * 16, 16), :]
            return 0

        lax.fori_loop(0, HALO // 16, put, 0)

        def permute(row, wt):
            at = row - sr + HALO
            for j in range(wt):
                v = GT[al(at + 8 * j, 8), :]
                if wt > 1:
                    FG[pl.ds(at + j, 8, stride=wt), :] = v
                else:
                    FG[al(at, 8), :] = v

        blocks(sr, srn + 16, permute)

    def out_copies():
        return [pltpu.make_async_copy(LOC.at[k, pl.ds(LOCPAD, LROWS)], out3.at[k], osem.at[k]) for k in range(3)]

    def finish3():
        back = lax.rem(128 - delta, 128)
        keep = lane < 128 - delta

        def one(i, _):
            for j in range(5):
                at = i * 40 + j * 8
                o = al(LOCPAD + at, 8)
                g = shift(FG, HALO + drow + at, 1, back, keep)
                new = adam(g, LOC[0, o, :], LOC[1, o, :], LOC[2, o, :], sc)
                for k in range(3):
                    LOC[k, o, :] = new[k]
            return 0

        lax.fori_loop(0, LROWS // 40, one, 0)
        for cp in out_copies():
            cp.start()

    for cp in state_copies():
        cp.start()
    for q in range(AHEAD):
        start0(q)

    def step(s, _):
        def at_stage(n, body):
            q = s - n

            @pl.when(jnp.logical_and(q >= 0, q < K))
            def _():
                body(q)

        def first(q):
            wait0(q)

            @pl.when(q + AHEAD < K)
            def _():
                start0(q + AHEAD)

            slot = lax.rem(q, S0)
            loop_add(lambda w: S.at[bits(w, 4) + (al(q * CH, CH),)], lambda w: R0.at[(slot,) + bits(w, 4)], 16, CH)
            for k in range(3):
                start(rs_copy(k, 0, q), q)

        at_stage(0, first)

        @pl.when(s == 1)
        def _():
            prepare1()

        for st in range(1, NST):
            def middle(q, st=st):
                for k in range(3):
                    reduce_stage(k, st - 1, q)
                    start(rs_copy(k, st, q), q)

            at_stage(st, middle)

        @pl.when(s == 2)
        def _():
            prepare2()

        def update(q):
            for k in range(3):
                reduce_stage(k, NST - 1, q)

            def one(i, _):
                o = al(q * CH + i * 16, 16)
                oh = al(HALO + q * CH + i * 16, 16)
                g = S[me + (o,)] * (1.0 / DEV)
                GT[oh, :] = g
                _, _, w2 = adam(g, TIL[0, oh, :], TIL[1, oh, :], TIL[2, oh, :], sc)
                WB[o, :] = w2.astype(BF16)
                return 0

            lax.fori_loop(0, CH // 16, one, 0)
            own_copy(q).start()
            for k in range(3):
                start(ag_copy(k, 0, q, False), q)

        at_stage(NST, update)

        for st in range(NST):
            def gather(q, st=st):
                if st == 0:
                    own_copy(q).wait()
                for k in range(3):
                    ag_copy(k, st, q, True).wait_recv()
                    if st + 1 < NST:
                        start(ag_copy(k, st + 1, q, False), q)
                    if st:
                        fw_copy(k, st - 1, q, 1 - c).wait_recv()
                    start(fw_copy(k, st, q, c), q)

            at_stage(NST + 1 + st, gather)

        def last(q):
            for k in range(3):
                fw_copy(k, NST - 1, q, 1 - c).wait_recv()

        at_stage(2 * NST + 1, last)

        for n, f in enumerate((finish1, finish2, finish3)):
            @pl.when(s == K + NST - 1 + n)
            def _(f=f):
                f()

        return 0

    lax.fori_loop(0, K + 2 * NST + 1, step, 0)

    def drain(i, _):
        q = K - SL + i
        for k in range(3):
            for st in range(NST):
                rs_copy(k, st, q).wait_send()
                ag_copy(k, st, q, False).wait_send()
                fw_copy(k, st, q, c).wait_send()
        return 0

    lax.fori_loop(0, SL, drain, 0)
    for cp in out_copies():
        cp.wait()


def unpack_kernel(ag, e_out, q_out, o_out, w1_out, w2_out, t_out, buf, isem, osem):
    outs = (e_out, q_out, o_out, w1_out, w2_out, t_out)
    depth = buf.shape[0]

    def get(r):
        return pltpu.make_async_copy(ag.at[tuple(r >> i & 1 for i in (4, 3, 2, 1, 0))], buf.at[r % depth], isem.at[r % depth])

    def puts(r):
        end = min(win_start(r + 1), TAIL0 + TAIL_ROWS) - win_start(r) if r + 1 < DEV else NR
        cps = []
        for n, (i, a, b, size) in enumerate(rows_of(r)):
            size = min(size, end - b)
            if size > 0:
                cps.append(pltpu.make_async_copy(buf.at[r % depth, pl.ds(b, size)], outs[i].at[pl.ds(a, size)],
                                                 osem.at[r % depth, n]))
        return cps

    for r in range(depth - 2):
        get(r).start()
    for r in range(DEV):
        get(r).wait()
        for cp in puts(r):
            cp.start()
        n = r + depth - 2
        if n < DEV:
            if n - depth >= 0:
                for cp in puts(n - depth):
                    cp.wait()
            get(n).start()
    for r in range(max(0, DEV - depth), DEV):
        for cp in puts(r):
            cp.wait()


def tiles(x, wt):
    rows = math.prod(x.shape) // (128 * wt)
    return x.reshape(rows // 8, 8, wt, 128).transpose(0, 2, 1, 3).reshape(rows * wt, 128)


def untiles(x, wt, shape):
    rows = x.shape[0] // wt
    return x.reshape(rows // 8, wt, 8, 128).transpose(0, 2, 1, 3).reshape(shape)


def solution(mesh):
    any_spec = pl.BlockSpec(memory_space=pl.ANY)
    dma = pltpu.SemaphoreType.DMA

    def vmem(*shape, dtype=F32):
        return pltpu.VMEM(shape + (128,), dtype)

    def body(g_emb, g_qkv, g_o, g_w1, g_w2, g_bqkv, g_b1, g_dvec, m, v, w, lr, beta1, beta2, eps, step):
        grads = (g_emb, g_qkv, g_o, g_w1, g_w2)
        shapes = tuple(g.shape[1:] for g in grads)
        big = [tiles(g, t[2]) for g, t in zip(grads, TENSORS)]
        tail = jnp.concatenate([g_bqkv.reshape(-1), g_b1.reshape(-1), g_dvec.reshape(-1)])
        tail = jnp.pad(tail, (0, TAIL_ROWS * 128 - tail.shape[0])).reshape(TAIL_ROWS, 128)
        t = step.astype(F32)
        sc = jnp.stack([lr, beta1, 1.0 - beta1, beta2, 1.0 - beta2,
                        1.0 / (1.0 - beta1 ** t), 1.0 / (1.0 - beta2 ** t), eps])
        state = [jnp.pad(a, (0, LROWS * 128 - SHARD)).reshape(LROWS, 128) for a in (m, v, w)]
        ag, out3 = pl.pallas_call(
            comm_kernel,
            out_shape=(jax.ShapeDtypeStruct((2, 2, 2, 2, 2, NR, 128), BF16), jax.ShapeDtypeStruct((3, LROWS, 128), F32)),
            in_specs=[pl.BlockSpec(memory_space=pltpu.SMEM)] + [any_spec] * 9,
            out_specs=(any_spec, any_spec),
            scratch_shapes=[vmem(SL, *[2] * (NST - 1 - st), n) for n in PARTS for st in range(NST)] + [
                vmem(2, 2, 2, 2, NR), vmem(S0, 2, 2, 2, 2, CH),
                vmem(3, 2176), vmem(3, FROWS), vmem(3, FROWS), vmem(3, HALO + 16), vmem(3, HALO + 16),
                vmem(NR + 2 * HALO), vmem(HALO), vmem(HALO + 16), vmem(NR + 2 * HALO), vmem(NR, dtype=BF16),
                dma((S0,)), dma((S0,)), dma((S0,))] + [dma((3, NST, SL)) for _ in range(6)] + [
                dma((SL,)), dma((3,)), dma((4,)), dma((4,)), dma((3,)),
            ],
            compiler_params=pltpu.CompilerParams(has_side_effects=True, vmem_limit_bytes=60 * 2 ** 20),
            name="reduce_adam_gather",
        )(sc, *big, tail, *state)
        outs = pl.pallas_call(
            unpack_kernel,
            out_shape=tuple(jax.ShapeDtypeStruct((b - a, 128), BF16) for a, b, _ in TENSORS)
            + (jax.ShapeDtypeStruct((TAIL_ROWS, 128), BF16),),
            in_specs=[any_spec],
            out_specs=(any_spec,) * 6,
            scratch_shapes=[pltpu.VMEM((12, NR, 128), BF16), dma((12,)), dma((12, 2))],
            compiler_params=pltpu.CompilerParams(vmem_limit_bytes=40 * 2 ** 20),
            name="unpack",
        )(ag)
        wb = [untiles(o, tt[2], s) for o, tt, s in zip(outs[:5], TENSORS, shapes)]
        flat = outs[5].reshape(-1)
        n1, n2 = g_bqkv.size, g_b1.size
        wb += [flat[:n1].reshape(g_bqkv.shape[1:]), flat[n1:n1 + n2].reshape(g_b1.shape[1:]),
               flat[n1 + n2:n1 + n2 + g_dvec.size].reshape(g_dvec.shape[1:])]
        new = [out3[k].reshape(-1)[:SHARD] for k in range(3)]
        return tuple(new) + tuple(wb)

    g3 = P(AXES, None, None)
    g4 = P(AXES, None, None, None)
    flat = P(AXES)
    rep = P()
    in_specs = (g3, g4, g4, g4, g4, g3, g3, g4, flat, flat, flat, rep, rep, rep, rep, rep)
    out_specs = (flat, flat, flat, rep, rep, rep, rep, rep, rep, rep, rep)
    return jax.shard_map(body, mesh=mesh, in_specs=in_specs, out_specs=out_specs, check_vma=False)
```

```python
import functools
import math

import jax
import jax.numpy as jnp
from jax import lax
from jax.experimental import pallas as pl
from jax.experimental.pallas import tpu as pltpu
from jax.sharding import PartitionSpec as P

AXES = ("outer", "inner")
MESH = pl.DeviceIdType.MESH
F32 = jnp.float32
BF16 = jnp.bfloat16

DEV = 32
SHARD = 270616
ROWS16 = 33827
TENSORS = ((0, 24576, 6), (24576, 38400, 18), (38400, 43008, 6), (43008, 55296, 16), (55296, 67584, 6))
TAIL0 = 67584
TAIL_ROWS = 80
LAST_ROW = 67654
NR = 2128
K = 19
NA, NB, NC = 40, 48, 24
CH = NA + NB + NC
SL = 4
S0 = 5
AHEAD = 2
HALO = 160
LOCPAD = 24
LROWS = 2120
FROWS = 2464
SROWS = 2176


def win_start(r):
    if isinstance(r, int):
        return (r * ROWS16) // 256 * 16
    return lax.div(r * ROWS16, 256) * 16


def rows_of(r):
    lo, hi = win_start(r), win_start(r) + NR
    segs = []
    for i, (a, b, _) in enumerate(TENSORS + ((TAIL0, TAIL0 + TAIL_ROWS, 1),)):
        s, e = max(lo, a), min(hi, b)
        if s < e:
            segs.append((i, s - a, s - lo, e - s))
    return segs


def al(i, n, a=8):
    return pl.ds(pl.multiple_of(i, a), n)


def bits(w, n):
    out = []
    for _ in range(n):
        out.append(lax.rem(w, 2))
        w = lax.div(w, 2)
    return tuple(out[::-1])


def loop_add(dst, src, lead, n):
    def one(w, _):
        d, s = dst(w), src(w)
        for o in range(0, n, 8):
            d[pl.ds(o, 8), :] = d[pl.ds(o, 8), :] + s[pl.ds(o, 8), :]
        return 0

    lax.fori_loop(0, lead, one, 0)


def adam(g, m, v, w, sc):
    lr, b1, c1, b2, c2, i1, i2, eps = sc
    m2 = b1 * m + c1 * g
    v2 = b2 * v + c2 * (g * g)
    w2 = w - lr * (m2 * i1) / (jnp.sqrt(v2 * i2) + eps)
    return m2, v2, w2


H, L, Y, X = range(4)
ORDERS = ((X, Y, L, H), (Y, X, L, H), (L, H, X, Y))
PARTS = (NA, NB, NC)
STARTS = (0, NA, NA + NB)
NST = len(ORDERS[0])


def comm_kernel(sc_ref, e_ref, q_ref, o_ref, w1_ref, w2_ref, t_ref, m_ref, v_ref, w_ref, ag, m_out, v_out, w_out, *scratch):
    bufs, scratch = scratch[:3 * NST], scratch[3 * NST:]
    (S, R0, F, TIL, HP, HN, GT, GP, GN, FG,
     ld, s0s, s0r, rss, rsr, ags, agr, fws, fwr, hs, hr) = scratch
    z = lax.axis_index(AXES[0])
    inner = lax.axis_index(AXES[1])
    h, l, y, x, c = bits(z, 2) + bits(inner, 3)
    me = (h, l, y, x)
    r = z * 8 + inner
    g_refs = (e_ref, q_ref, o_ref, w1_ref, w2_ref, t_ref)
    sc = [sc_ref[i] for i in range(8)]
    state = (m_ref, v_ref, w_ref)

    def flip(ax):
        p = [1 - b if i == ax else b for i, b in enumerate(me)]
        return p[H] * 2 + p[L], p[Y] * 4 + p[X] * 2 + c

    PEER = [flip(ax) for ax in range(4)]
    CORE = (z, inner + 1 - 2 * c)

    def device(i):
        i = lax.rem(i, DEV)
        return lax.div(i, 8), lax.rem(i, 8)

    NXT, PRV = device(r + 1), device(r + DEV - 1)

    def remote(src, dst, ss, rs, dev):
        return pltpu.make_async_remote_copy(src_ref=src, dst_ref=dst, send_sem=ss, recv_sem=rs,
                                            device_id=dev, device_id_type=MESH)

    def window_copies(w, q, make):
        segs = rows_of(w)
        off = q * CH
        if len(segs) == 1:
            i, a, _, _ = segs[0]
            make(g_refs[i].at[al(a + off, CH)], 0, CH)
            return
        for n, (i, a, b, size) in enumerate(segs):
            first, last = -(-b // CH), (b + size) // CH

            @pl.when(jnp.logical_and(q >= first, q < last))
            def _(i=i, a=a, b=b):
                make(g_refs[i].at[al(jnp.maximum(a + off - b, 0), CH)], 0, CH)

            if n + 1 < len(segs) and (b + size) % CH:
                edge, head = (b + size) // CH, (b + size) % CH
                j, a2, _, _ = segs[n + 1]

                @pl.when(q == edge)
                def _(i=i, a=a, size=size, head=head, j=j, a2=a2):
                    make(g_refs[i].at[pl.ds(a + size - head, head)], 0, head)
                    make(g_refs[j].at[pl.ds(a2, CH - head)], head, CH - head)

    def start0(q):
        slot = lax.rem(q, S0)
        for par in range(2):

            @pl.when(c == par)
            def _(par=par):
                for k in range(16):
                    idx = tuple(k >> i & 1 for i in (3, 2, 1, 0))

                    def send(src, o, n, idx=idx):
                        remote(src, R0.at[(slot,) + idx + (pl.ds(o, n),)], s0s.at[slot], s0r.at[slot], CORE).start()

                    def load(src, o, n, idx=idx):
                        pltpu.make_async_copy(src, S.at[idx + (al(q * CH + o, n),)], ld.at[slot]).start()

                    window_copies(2 * k + 1 - par, q, send)
                    window_copies(2 * k + par, q, load)

    def wait0(q):
        slot = lax.rem(q, S0)
        rows = S.at[:, :, :, :, al(q * CH, CH)]
        pltpu.make_async_copy(rows, rows, ld.at[slot]).wait()
        remote(R0.at[slot], R0.at[slot], s0s.at[slot], s0r.at[slot], CORE).wait()

    every = slice(None)

    def part(k, q):
        return al(q * CH + STARTS[k], PARTS[k])

    def where_rs(k, st, q, other):
        o = ORDERS[k]
        idx = [every] * 4
        for ax in o[:st]:
            idx[ax] = me[ax]
        idx[o[st]] = 1 - me[o[st]] if other else me[o[st]]
        return idx + [part(k, q)]

    def where_ag(k, st, q, other, core):
        o = ORDERS[k][::-1]
        idx = list(me)
        for ax in o[:st]:
            idx[ax] = every
        idx[o[st]] = 1 - me[o[st]] if other else me[o[st]]
        return tuple(idx + [core, part(k, q)])

    def rs_copy(k, st, q):
        s = lax.rem(q, SL)
        return remote(S.at[tuple(where_rs(k, st, q, True))], bufs[k * NST + st].at[s],
                      rss.at[k, st, s], rsr.at[k, st, s], PEER[ORDERS[k][st]])

    def ag_copy(k, st, q, recv):
        s = lax.rem(q, SL)
        dst = ag.at[where_ag(k, st, q, recv, c)]
        return remote(dst, dst, ags.at[k, st, s], agr.at[k, st, s], PEER[ORDERS[k][NST - 1 - st]])

    def fw_copy(k, st, q, core):
        s = lax.rem(q, SL)
        idx = list(where_ag(k, st, q, True, core))
        if st == 0:
            idx[ORDERS[k][NST - 1]] = every
        ref = ag.at[tuple(idx)]
        return remote(ref, ref, fws.at[k, st, s], fwr.at[k, st, s], CORE)

    def start(cp, q):
        @pl.when(q >= SL)
        def _():
            cp.wait_send()

        cp.start()

    def reduce_stage(k, st, q):
        rs_copy(k, st, q).wait_recv()
        s = lax.rem(q, SL)
        idx = where_rs(k, st, q, False)
        free = ORDERS[k][st + 1:]

        def dst(w):
            at = list(idx)
            for ax, b in zip(sorted(free), bits(w, len(free))):
                at[ax] = b
            return S.at[tuple(at)]

        loop_add(dst, lambda w: bufs[k * NST + st].at[(s,) + bits(w, len(free))], 2 ** len(free), PARTS[k])

    sr, srn = win_start(r), win_start(r + 1)
    delta = lax.rem(r * 24, 128)
    drow = lax.div(r * ROWS16, 16) - sr
    edge_n = lax.rem((r + 1) * 24, 128) + 128 * (lax.div((r + 1) * ROWS16, 16) - srn)
    nb = HALO + srn - sr
    lane = lax.broadcasted_iota(jnp.int32, (8, 128), 1)
    sub = lax.broadcasted_iota(jnp.int32, (8, 128), 0)

    def halo_copies():
        return [remote(F.at[:, al(nb - HALO, HALO + 16)], HP, hs.at[0], hr.at[0], NXT),
                remote(F.at[:, pl.ds(HALO, HALO + 16)], HN, hs.at[1], hr.at[1], PRV)]

    def shift(ref, at, other, by, keep):
        return pltpu.roll(jnp.where(keep, ref[pl.ds(at, 8), :], ref[pl.ds(at + other, 8), :]), by, 1)

    def prepare1(lo, hi):
        keep = lane < 128 - delta

        def one(i, _):
            for j in range(4):
                at = i * 32 + j * 8
                for k in range(3):
                    F[k, al(HALO + at, 8), :] = shift(state[k], LOCPAD + at - drow, -1, delta, keep)
            return 0

        lax.fori_loop(lo, hi, one, 0)

    def blocks(first, last, body):
        for a, b, wt in TENSORS + ((TAIL0, TAIL0 + TAIL_ROWS, 1),):
            lo = lax.div(jnp.maximum(first - a, 0), 8 * wt)
            hi = lax.div(jnp.maximum(jnp.minimum(last, b) - a, 0) + 8 * wt - 1, 8 * wt)

            def one(i, _, a=a, wt=wt):
                body(a + i * 8 * wt, wt)
                return 0

            lax.fori_loop(lo, hi, one, 0)

    def prepare2():
        for cp in halo_copies():
            cp.wait()
        for k in range(3):
            for i in range(0, 16, 8):
                idx = (sub + i) * 128 + lane
                o = pl.ds(HALO + i, 8)
                F[k, o, :] = jnp.where(idx < drow * 128 + delta, HP[k, o, :], F[k, o, :])
                o = al(nb + i, 8)
                F[k, o, :] = jnp.where(idx >= edge_n, HN[k, pl.ds(i, 8), :], F[k, o, :])

        def one(i, _):
            for k in range(3):
                F[k, al(i * 16, 16), :] = HP[k, al(i * 16, 16), :]
                F[k, al(nb + 16 + i * 16, 16), :] = HN[k, al(16 + i * 16, 16), :]
            return 0

        lax.fori_loop(0, HALO // 16, one, 0)

    def prepare3(ks):
        def permute(row, wt):
            at = row - sr + HALO
            for j in range(wt):
                for k in ks:
                    TIL[k, al(at + 8 * j, 8), :] = (
                        F[k, pl.ds(at + j, 8, stride=wt), :] if wt > 1 else F[k, al(at, 8), :])

        blocks(sr, sr + NR, permute)

    def ghalo_copies():
        return [remote(GT.at[al(nb - HALO, HALO)], GP, hs.at[2], hr.at[2], NXT),
                remote(GT.at[pl.ds(HALO, HALO + 16)], GN, hs.at[3], hr.at[3], PRV)]

    def finish2():
        for cp in ghalo_copies():
            cp.wait()

        def put(i, _):
            GT[al(i * 16, 16), :] = GP[al(i * 16, 16), :]
            GT[al(HALO + NR + i * 16, 16), :] = GN[al(HALO + NR - nb + i * 16, 16), :]
            return 0

        lax.fori_loop(0, HALO // 16, put, 0)

        def permute(row, wt):
            at = row - sr + HALO
            for j in range(wt):
                v = GT[al(at + 8 * j, 8), :]
                if wt > 1:
                    FG[pl.ds(at + j, 8, stride=wt), :] = v
                else:
                    FG[al(at, 8), :] = v

        blocks(sr, srn + 16, permute)

    def finish3(lo, hi):
        back = lax.rem(128 - delta, 128)

        def one(i, _):
            for j in range(5):
                at = i * 40 + j * 8
                g = shift(FG, HALO + drow + at, 1, back, lane >= delta)
                new = adam(g, *[ref[al(LOCPAD + at, 8), :] for ref in state], sc)
                for ref, val in zip((m_out, v_out, w_out), new):
                    ref[al(at, 8), :] = val
            return 0

        lax.fori_loop(lo, hi, one, 0)

    for q in range(AHEAD):
        start0(q)

    def step(s, _):
        def at_stage(n, body):
            q = s - n

            @pl.when(jnp.logical_and(q >= 0, q < K))
            def _():
                body(q)

        def first(q):
            wait0(q)

            @pl.when(q + AHEAD < K)
            def _():
                start0(q + AHEAD)

            slot = lax.rem(q, S0)
            loop_add(lambda w: S.at[bits(w, 4) + (al(q * CH, CH),)], lambda w: R0.at[(slot,) + bits(w, 4)], 16, CH)
            for k in range(3):
                start(rs_copy(k, 0, q), q)

        at_stage(0, first)

        for st in range(1, NST):
            def middle(q, st=st):
                for k in range(3):
                    reduce_stage(k, st - 1, q)
                    start(rs_copy(k, st, q), q)

            at_stage(st, middle)

        def update(q):
            for k in range(3):
                reduce_stage(k, NST - 1, q)

            def one(i, _):
                o = al(q * CH + i * 16, 16)
                oh = al(HALO + q * CH + i * 16, 16)
                g = S[me + (o,)] * (1.0 / DEV)
                GT[oh, :] = g
                _, _, w2 = adam(g, TIL[0, oh, :], TIL[1, oh, :], TIL[2, oh, :], sc)
                ag[me + (c, o)] = w2.astype(BF16)
                return 0

            lax.fori_loop(0, CH // 16, one, 0)
            for k in range(3):
                start(ag_copy(k, 0, q, False), q)

        at_stage(NST, update)

        for st in range(NST):
            def gather(q, st=st):
                for k in range(3):
                    ag_copy(k, st, q, True).wait_recv()
                    if st + 1 < NST:
                        start(ag_copy(k, st + 1, q, False), q)
                    if st:
                        fw_copy(k, st - 1, q, 1 - c).wait_recv()
                    start(fw_copy(k, st, q, c), q)

            at_stage(NST + 1 + st, gather)

        def last(q):
            for k in range(3):
                fw_copy(k, NST - 1, q, 1 - c).wait_recv()

        at_stage(2 * NST + 1, last)

        def send_halos(copies):
            for cp in copies():
                cp.start()

        half, done, outer = (NR + 16) // 64, K + NST - 1, LROWS // 40
        extra = {
            0: lambda: prepare1(0, half),
            1: lambda: (prepare1(half, (NR + 16) // 32), send_halos(halo_copies)),
            2: lambda: (prepare2(), prepare3((0,))),
            3: lambda: prepare3((1, 2)),
            done: lambda: send_halos(ghalo_copies),
            done + 1: finish2,
        }
        cuts = [outer * i // NST for i in range(NST + 1)]
        for i in range(NST):
            extra[done + 2 + i] = lambda i=i: finish3(cuts[i], cuts[i + 1])
        for n, f in extra.items():
            @pl.when(s == n)
            def _(f=f):
                f()

        return 0

    lax.fori_loop(0, K + 2 * NST + 1, step, 0)

    def drain(i, _):
        q = K - SL + i
        for k in range(3):
            for st in range(NST):
                rs_copy(k, st, q).wait_send()
                ag_copy(k, st, q, False).wait_send()
                fw_copy(k, st, q, c).wait_send()
        return 0

    lax.fori_loop(0, SL, drain, 0)


def unpack_kernel(ag, e_out, q_out, o_out, w1_out, w2_out, t_out, sem):
    outs = (e_out, q_out, o_out, w1_out, w2_out, t_out)
    cps = []
    for r in range(DEV):
        end = min(win_start(r + 1), TAIL0 + TAIL_ROWS) - win_start(r) if r + 1 < DEV else NR
        for i, a, b, size in rows_of(r):
            size = min(size, end - b)
            if size > 0:
                src = ag.at[tuple(r >> j & 1 for j in (4, 3, 2, 1, 0)) + (pl.ds(b, size),)]
                cps.append(pltpu.make_async_copy(src, outs[i].at[pl.ds(a, size)], sem.at[len(cps)]))
    for cp in cps:
        cp.start()
    for cp in cps:
        cp.wait()


def tiles(x, wt):
    rows = math.prod(x.shape) // (128 * wt)
    return x.reshape(rows // 8, 8, wt, 128).transpose(0, 2, 1, 3).reshape(rows * wt, 128)


def untiles(x, wt, shape):
    rows = x.shape[0] // wt
    return x.reshape(rows // 8, wt, 8, 128).transpose(0, 2, 1, 3).reshape(shape)


def solution(mesh):
    any_spec = pl.BlockSpec(memory_space=pl.ANY)
    vmem_spec = pl.BlockSpec(memory_space=pltpu.VMEM)
    dma = pltpu.SemaphoreType.DMA

    def vmem(*shape, dtype=F32):
        return pltpu.VMEM(shape + (128,), dtype)

    def body(g_emb, g_qkv, g_o, g_w1, g_w2, g_bqkv, g_b1, g_dvec, m, v, w, lr, beta1, beta2, eps, step):
        grads = (g_emb, g_qkv, g_o, g_w1, g_w2)
        shapes = tuple(g.shape[1:] for g in grads)
        big = [tiles(g, t[2]) for g, t in zip(grads, TENSORS)]
        tail = jnp.concatenate([g_bqkv.reshape(-1), g_b1.reshape(-1), g_dvec.reshape(-1)])
        tail = jnp.pad(tail, (0, TAIL_ROWS * 128 - tail.shape[0])).reshape(TAIL_ROWS, 128)
        t = step.astype(F32)
        sc = jnp.stack([lr, beta1, 1.0 - beta1, beta2, 1.0 - beta2,
                        1.0 / (1.0 - beta1 ** t), 1.0 / (1.0 - beta2 ** t), eps])
        front = LOCPAD * 128
        state = [pltpu.with_memory_space_constraint(
            jnp.pad(a, (front, SROWS * 128 - front - SHARD)).reshape(SROWS, 128), pltpu.VMEM) for a in (m, v, w)]
        ag, *new = pl.pallas_call(
            comm_kernel,
            out_shape=(pltpu.VMEM((2, 2, 2, 2, 2, NR, 128), BF16),) + (pltpu.VMEM((LROWS, 128), F32),) * 3,
            in_specs=[pl.BlockSpec(memory_space=pltpu.SMEM)] + [any_spec] * 6 + [vmem_spec] * 3,
            out_specs=(vmem_spec,) * 4,
            scratch_shapes=[vmem(SL, *[2] * (NST - 1 - st), n) for n in PARTS for st in range(NST)] + [
                vmem(2, 2, 2, 2, NR), vmem(S0, 2, 2, 2, 2, CH),
                vmem(3, FROWS), vmem(3, FROWS), vmem(3, HALO + 16), vmem(3, HALO + 16),
                vmem(NR + 2 * HALO), vmem(HALO), vmem(HALO + 16), vmem(NR + 2 * HALO),
                dma((S0,)), dma((S0,)), dma((S0,))] + [dma((3, NST, SL)) for _ in range(6)] + [
                dma((4,)), dma((4,)),
            ],
            compiler_params=pltpu.CompilerParams(has_side_effects=True, vmem_limit_bytes=36 * 2 ** 20),
            name="reduce_adam_gather",
        )(sc, *big, tail, *state)
        outs = pl.pallas_call(
            unpack_kernel,
            out_shape=tuple(jax.ShapeDtypeStruct((b - a, 128), BF16) for a, b, _ in TENSORS)
            + (jax.ShapeDtypeStruct((TAIL_ROWS, 128), BF16),),
            in_specs=[vmem_spec],
            out_specs=(any_spec,) * 6,
            scratch_shapes=[dma((DEV + 8,))],
            compiler_params=pltpu.CompilerParams(vmem_limit_bytes=20 * 2 ** 20),
            name="unpack",
        )(ag)
        wb = [untiles(o, tt[2], s) for o, tt, s in zip(outs[:5], TENSORS, shapes)]
        flat = outs[5].reshape(-1)
        n1, n2 = g_bqkv.size, g_b1.size
        wb += [flat[:n1].reshape(g_bqkv.shape[1:]), flat[n1:n1 + n2].reshape(g_b1.shape[1:]),
               flat[n1 + n2:n1 + n2 + g_dvec.size].reshape(g_dvec.shape[1:])]
        new = [a.reshape(-1)[:SHARD] for a in new]
        return tuple(new) + tuple(wb)

    g3 = P(AXES, None, None)
    g4 = P(AXES, None, None, None)
    flat = P(AXES)
    rep = P()
    in_specs = (g3, g4, g4, g4, g4, g3, g3, g4, flat, flat, flat, rep, rep, rep, rep, rep)
    out_specs = (flat, flat, flat, rep, rep, rep, rep, rep, rep, rep, rep)
    return jax.shard_map(body, mesh=mesh, in_specs=in_specs, out_specs=out_specs, check_vma=False)
```

```python
import functools
import math

import jax
import jax.numpy as jnp
from jax import lax
from jax.experimental import pallas as pl
from jax.experimental.pallas import tpu as pltpu
from jax.sharding import PartitionSpec as P

AXES = ("outer", "inner")
MESH = pl.DeviceIdType.MESH
F32 = jnp.float32
BF16 = jnp.bfloat16

DEV = 32
SHARD = 270616
ROWS16 = 33827
TENSORS = ((0, 24576, 6), (24576, 38400, 18), (38400, 43008, 6), (43008, 55296, 16), (55296, 67584, 6))
TAIL0 = 67584
TAIL_ROWS = 80
LAST_ROW = 67654
NR = 2128
K = 19
NA, NB, NC = 40, 48, 24
CH = NA + NB + NC
SL = 4
S0 = 5
AHEAD = 2
HALO = 160
LOCPAD = 24
LROWS = 2120
FROWS = 2464
SROWS = 2176


def win_start(r):
    if isinstance(r, int):
        return (r * ROWS16) // 256 * 16
    return lax.div(r * ROWS16, 256) * 16


def rows_of(r):
    lo, hi = win_start(r), win_start(r) + NR
    segs = []
    for i, (a, b, _) in enumerate(TENSORS + ((TAIL0, TAIL0 + TAIL_ROWS, 1),)):
        s, e = max(lo, a), min(hi, b)
        if s < e:
            segs.append((i, s - a, s - lo, e - s))
    return segs


def halo_rows(n):
    s = win_start(n)
    for a, b, wt in TENSORS + ((TAIL0, TAIL0 + TAIL_ROWS, 1),):
        if a <= s < b:
            first = a + (s - a) // (8 * wt) * 8 * wt
            end = first + 8 * wt
    return s + 16 - first // 16 * 16, max(16, -(-end // 16) * 16 - s) if first < s else 16


def al(i, n, a=8):
    return pl.ds(pl.multiple_of(i, a), n)


def bits(w, n):
    out = []
    for _ in range(n):
        out.append(lax.rem(w, 2))
        w = lax.div(w, 2)
    return tuple(out[::-1])


def loop_add(dst, src, lead, n):
    def one(w, _):
        d, s = dst(w), src(w)
        for o in range(0, n, 8):
            d[pl.ds(o, 8), :] = d[pl.ds(o, 8), :] + s[pl.ds(o, 8), :]
        return 0

    lax.fori_loop(0, lead, one, 0)


def adam(g, m, v, w, sc):
    lr, b1, c1, b2, c2, i1, i2, eps = sc
    m2 = b1 * m + c1 * g
    v2 = b2 * v + c2 * (g * g)
    w2 = w - lr * (m2 * i1) / (jnp.sqrt(v2 * i2) + eps)
    return m2, v2, w2


H, L, Y, X = range(4)
ORDERS = ((X, Y, L, H), (Y, X, L, H), (L, H, X, Y))
PARTS = (NA, NB, NC)
STARTS = (0, NA, NA + NB)
NST = len(ORDERS[0])


def comm_kernel(sc_ref, e_ref, q_ref, o_ref, w1_ref, w2_ref, t_ref, m_ref, v_ref, w_ref, ag, m_out, v_out, w_out, *scratch):
    bufs, scratch = scratch[:3 * NST], scratch[3 * NST:]
    (S, R0, F, TIL, HP, HN, GT, GP, GN, FG,
     ld, s0s, s0r, rss, rsr, ags, agr, fws, fwr, hs, hr) = scratch
    z = lax.axis_index(AXES[0])
    inner = lax.axis_index(AXES[1])
    h, l, y, x, c = bits(z, 2) + bits(inner, 3)
    me = (h, l, y, x)
    r = z * 8 + inner
    g_refs = (e_ref, q_ref, o_ref, w1_ref, w2_ref, t_ref)
    sc = [sc_ref[i] for i in range(8)]
    state = (m_ref, v_ref, w_ref)

    def flip(ax):
        p = [1 - b if i == ax else b for i, b in enumerate(me)]
        return p[H] * 2 + p[L], p[Y] * 4 + p[X] * 2 + c

    PEER = [flip(ax) for ax in range(4)]
    CORE = (z, inner + 1 - 2 * c)

    def device(i):
        i = lax.rem(i, DEV)
        return lax.div(i, 8), lax.rem(i, 8)

    NXT, PRV = device(r + 1), device(r + DEV - 1)

    def remote(src, dst, ss, rs, dev):
        return pltpu.make_async_remote_copy(src_ref=src, dst_ref=dst, send_sem=ss, recv_sem=rs,
                                            device_id=dev, device_id_type=MESH)

    def window_copies(w, q, make):
        segs = rows_of(w)
        off = q * CH
        if len(segs) == 1:
            i, a, _, _ = segs[0]
            make(g_refs[i].at[al(a + off, CH)], 0, CH)
            return
        for n, (i, a, b, size) in enumerate(segs):
            first, last = -(-b // CH), (b + size) // CH

            @pl.when(jnp.logical_and(q >= first, q < last))
            def _(i=i, a=a, b=b):
                make(g_refs[i].at[al(jnp.maximum(a + off - b, 0), CH)], 0, CH)

            if n + 1 < len(segs) and (b + size) % CH:
                edge, head = (b + size) // CH, (b + size) % CH
                j, a2, _, _ = segs[n + 1]

                @pl.when(q == edge)
                def _(i=i, a=a, size=size, head=head, j=j, a2=a2):
                    make(g_refs[i].at[pl.ds(a + size - head, head)], 0, head)
                    make(g_refs[j].at[pl.ds(a2, CH - head)], head, CH - head)

    def start0(q):
        slot = lax.rem(q, S0)
        for par in range(2):

            @pl.when(c == par)
            def _(par=par):
                for k in range(16):
                    idx = tuple(k >> i & 1 for i in (3, 2, 1, 0))

                    def send(src, o, n, idx=idx):
                        remote(src, R0.at[(slot,) + idx + (pl.ds(o, n),)], s0s.at[slot], s0r.at[slot], CORE).start()

                    def load(src, o, n, idx=idx):
                        pltpu.make_async_copy(src, S.at[idx + (al(q * CH + o, n),)], ld.at[slot]).start()

                    window_copies(2 * k + 1 - par, q, send)
                    window_copies(2 * k + par, q, load)

    def wait0(q):
        slot = lax.rem(q, S0)
        rows = S.at[:, :, :, :, al(q * CH, CH)]
        pltpu.make_async_copy(rows, rows, ld.at[slot]).wait()
        remote(R0.at[slot], R0.at[slot], s0s.at[slot], s0r.at[slot], CORE).wait()

    every = slice(None)

    def part(k, q):
        return al(q * CH + STARTS[k], PARTS[k])

    def where_rs(k, st, q, other):
        o = ORDERS[k]
        idx = [every] * 4
        for ax in o[:st]:
            idx[ax] = me[ax]
        idx[o[st]] = 1 - me[o[st]] if other else me[o[st]]
        return idx + [part(k, q)]

    def where_ag(k, st, q, other, core):
        o = ORDERS[k][::-1]
        idx = list(me)
        for ax in o[:st]:
            idx[ax] = every
        idx[o[st]] = 1 - me[o[st]] if other else me[o[st]]
        return tuple(idx + [core, part(k, q)])

    def rs_copy(k, st, q):
        s = lax.rem(q, SL)
        return remote(S.at[tuple(where_rs(k, st, q, True))], bufs[k * NST + st].at[s],
                      rss.at[k, st, s], rsr.at[k, st, s], PEER[ORDERS[k][st]])

    def ag_copy(k, st, q, recv):
        s = lax.rem(q, SL)
        dst = ag.at[where_ag(k, st, q, recv, c)]
        return remote(dst, dst, ags.at[k, st, s], agr.at[k, st, s], PEER[ORDERS[k][NST - 1 - st]])

    def fw_copy(k, st, q, core):
        s = lax.rem(q, SL)
        idx = list(where_ag(k, st, q, True, core))
        if st == 0:
            idx[ORDERS[k][NST - 1]] = every
        ref = ag.at[tuple(idx)]
        return remote(ref, ref, fws.at[k, st, s], fwr.at[k, st, s], CORE)

    def start(cp, q):
        @pl.when(q >= SL)
        def _():
            cp.wait_send()

        cp.start()

    def reduce_stage(k, st, q):
        rs_copy(k, st, q).wait_recv()
        s = lax.rem(q, SL)
        idx = where_rs(k, st, q, False)
        free = ORDERS[k][st + 1:]

        def dst(w):
            at = list(idx)
            for ax, b in zip(sorted(free), bits(w, len(free))):
                at[ax] = b
            return S.at[tuple(at)]

        loop_add(dst, lambda w: bufs[k * NST + st].at[(s,) + bits(w, len(free))], 2 ** len(free), PARTS[k])

    sr, srn = win_start(r), win_start(r + 1)
    delta = lax.rem(r * 24, 128)
    drow = lax.div(r * ROWS16, 16) - sr
    edge_n = lax.rem((r + 1) * 24, 128) + 128 * (lax.div((r + 1) * ROWS16, 16) - srn)
    nb = HALO + srn - sr
    lane = lax.broadcasted_iota(jnp.int32, (8, 128), 1)
    sub = lax.broadcasted_iota(jnp.int32, (8, 128), 0)

    def halo_up(n):
        size, _ = halo_rows(n)
        o = pl.ds(HALO + 16 - size, size)
        return remote(F.at[:, al(nb + 16 - size, size)], HP.at[:, o], hs.at[0], hr.at[0], NXT)

    def halo_down(n):
        _, size = halo_rows(n)
        return remote(F.at[:, pl.ds(HALO, size)], HN.at[:, pl.ds(0, size)], hs.at[1], hr.at[1], PRV)

    def halos(sent, received):
        for n in range(DEV):
            @pl.when(r == n)
            def _(n=n):
                for cp in [halo_up(n + 1)] * (n + 1 < DEV) + [halo_down(n)] * (n > 0):
                    sent(cp)
                if received is not None:
                    for cp in [halo_down(n + 1)] * (n + 1 < DEV) + [halo_up(n)] * (n > 0):
                        received(cp)

    def shift(ref, at, other, by, keep):
        return pltpu.roll(jnp.where(keep, ref[pl.ds(at, 8), :], ref[pl.ds(at + other, 8), :]), by, 1)

    def prepare1(lo, hi):
        keep = lane < 128 - delta

        def one(i, _):
            for j in range(4):
                at = i * 32 + j * 8
                for k in range(3):
                    F[k, al(HALO + at, 8), :] = shift(state[k], LOCPAD + at - drow, -1, delta, keep)
            return 0

        lax.fori_loop(lo, hi, one, 0)

    def blocks(first, last, body):
        for a, b, wt in TENSORS + ((TAIL0, TAIL0 + TAIL_ROWS, 1),):
            lo = lax.div(jnp.maximum(first - a, 0), 8 * wt)
            hi = lax.div(jnp.maximum(jnp.minimum(last, b) - a, 0) + 8 * wt - 1, 8 * wt)

            def one(i, _, a=a, wt=wt):
                body(a + i * 8 * wt, wt)
                return 0

            lax.fori_loop(lo, hi, one, 0)

    def prepare2():
        halos(lambda cp: cp.wait_send(), lambda cp: cp.wait_recv())
        for k in range(3):
            for i in range(0, 16, 8):
                idx = (sub + i) * 128 + lane
                o = pl.ds(HALO + i, 8)
                F[k, o, :] = jnp.where(idx < drow * 128 + delta, HP[k, o, :], F[k, o, :])
                o = al(nb + i, 8)
                F[k, o, :] = jnp.where(idx >= edge_n, HN[k, pl.ds(i, 8), :], F[k, o, :])

        def one(i, _):
            for k in range(3):
                F[k, al(i * 16, 16), :] = HP[k, al(i * 16, 16), :]
                F[k, al(nb + 16 + i * 16, 16), :] = HN[k, al(16 + i * 16, 16), :]
            return 0

        lax.fori_loop(0, HALO // 16, one, 0)

    def prepare3(ks):
        def permute(row, wt):
            at = row - sr + HALO
            for j in range(wt):
                for k in ks:
                    TIL[k, al(at + 8 * j, 8), :] = (
                        F[k, pl.ds(at + j, 8, stride=wt), :] if wt > 1 else F[k, al(at, 8), :])

        blocks(sr, sr + NR, permute)

    def ghalo_copies():
        return [remote(GT.at[al(nb - HALO, HALO)], GP, hs.at[2], hr.at[2], NXT),
                remote(GT.at[pl.ds(HALO, HALO + 16)], GN, hs.at[3], hr.at[3], PRV)]

    def finish2():
        for cp in ghalo_copies():
            cp.wait()

        def put(i, _):
            GT[al(i * 16, 16), :] = GP[al(i * 16, 16), :]
            GT[al(HALO + NR + i * 16, 16), :] = GN[al(HALO + NR - nb + i * 16, 16), :]
            return 0

        lax.fori_loop(0, HALO // 16, put, 0)

        def permute(row, wt):
            at = row - sr + HALO
            for j in range(wt):
                v = GT[al(at + 8 * j, 8), :]
                if wt > 1:
                    FG[pl.ds(at + j, 8, stride=wt), :] = v
                else:
                    FG[al(at, 8), :] = v

        blocks(sr, srn + 16, permute)

    def finish3(lo, hi):
        back = lax.rem(128 - delta, 128)

        def one(i, _):
            for j in range(5):
                at = i * 40 + j * 8
                g = shift(FG, HALO + drow + at, 1, back, lane >= delta)
                new = adam(g, *[ref[al(LOCPAD + at, 8), :] for ref in state], sc)
                for ref, val in zip((m_out, v_out, w_out), new):
                    ref[al(at, 8), :] = val
            return 0

        lax.fori_loop(lo, hi, one, 0)

    barrier = pltpu.get_barrier_semaphore()
    friends = PEER + [CORE, NXT, PRV]
    for dev in friends:
        pl.semaphore_signal(barrier, inc=1, device_id=dev, device_id_type=MESH)
    pl.semaphore_wait(barrier, len(friends))
    for q in range(AHEAD):
        start0(q)
    turns, edge_turns = (NR + 16) // 32, (HALO + 32) // 32
    prepare1(0, edge_turns)
    prepare1(turns - edge_turns, turns)
    halos(lambda cp: cp.start(), None)

    def step(s, _):
        def at_stage(n, body):
            q = s - n

            @pl.when(jnp.logical_and(q >= 0, q < K))
            def _():
                body(q)

        def first(q):
            wait0(q)

            @pl.when(q + AHEAD < K)
            def _():
                start0(q + AHEAD)

            slot = lax.rem(q, S0)
            loop_add(lambda w: S.at[bits(w, 4) + (al(q * CH, CH),)], lambda w: R0.at[(slot,) + bits(w, 4)], 16, CH)
            for k in range(3):
                start(rs_copy(k, 0, q), q)

        at_stage(0, first)

        for st in range(1, NST):
            def middle(q, st=st):
                for k in range(3):
                    reduce_stage(k, st - 1, q)
                    start(rs_copy(k, st, q), q)

            at_stage(st, middle)

        def update(q):
            for k in range(3):
                reduce_stage(k, NST - 1, q)

            def one(i, _):
                o = al(q * CH + i * 16, 16)
                oh = al(HALO + q * CH + i * 16, 16)
                g = S[me + (o,)] * (1.0 / DEV)
                GT[oh, :] = g
                _, _, w2 = adam(g, TIL[0, oh, :], TIL[1, oh, :], TIL[2, oh, :], sc)
                ag[me + (c, o)] = w2.astype(BF16)
                return 0

            lax.fori_loop(0, CH // 16, one, 0)
            for k in range(3):
                start(ag_copy(k, 0, q, False), q)

        at_stage(NST, update)

        for st in range(NST):
            def gather(q, st=st):
                for k in range(3):
                    ag_copy(k, st, q, True).wait_recv()
                    if st + 1 < NST:
                        start(ag_copy(k, st + 1, q, False), q)
                    if st:
                        fw_copy(k, st - 1, q, 1 - c).wait_recv()
                    start(fw_copy(k, st, q, c), q)

            at_stage(NST + 1 + st, gather)

        def last(q):
            for k in range(3):
                fw_copy(k, NST - 1, q, 1 - c).wait_recv()

        at_stage(2 * NST + 1, last)

        def send_halos():
            for cp in ghalo_copies():
                cp.start()

        done, outer = K + NST - 1, LROWS // 40
        extra = {
            0: lambda: prepare1(edge_turns, turns // 2),
            1: lambda: prepare1(turns // 2, turns - edge_turns),
            2: lambda: (prepare2(), prepare3((0,))),
            3: lambda: prepare3((1, 2)),
            done: send_halos,
            done + 1: finish2,
        }
        cuts = [outer * i // NST for i in range(NST + 1)]
        for i in range(NST):
            extra[done + 2 + i] = lambda i=i: finish3(cuts[i], cuts[i + 1])
        for n, f in extra.items():
            @pl.when(s == n)
            def _(f=f):
                f()

        return 0

    lax.fori_loop(0, K + 2 * NST + 1, step, 0)

    def drain(i, _):
        q = K - SL + i
        for k in range(3):
            for st in range(NST):
                rs_copy(k, st, q).wait_send()
                ag_copy(k, st, q, False).wait_send()
                fw_copy(k, st, q, c).wait_send()
        return 0

    lax.fori_loop(0, SL, drain, 0)


def unpack_kernel(ag, m_new, v_new, w_new, e_out, q_out, o_out, w1_out, w2_out, t_out, m_out, v_out, w_out, sem):
    outs = (e_out, q_out, o_out, w1_out, w2_out, t_out)
    cps = [pltpu.make_async_copy(src, dst, sem.at[DEV + 8 + k])
           for k, (src, dst) in enumerate(((m_new, m_out), (v_new, v_out), (w_new, w_out)))]
    for r in range(DEV):
        end = min(win_start(r + 1), TAIL0 + TAIL_ROWS) - win_start(r) if r + 1 < DEV else NR
        for i, a, b, size in rows_of(r):
            size = min(size, end - b)
            if size > 0:
                src = ag.at[tuple(r >> j & 1 for j in (4, 3, 2, 1, 0)) + (pl.ds(b, size),)]
                cps.append(pltpu.make_async_copy(src, outs[i].at[pl.ds(a, size)], sem.at[len(cps) - 3]))
    for cp in cps:
        cp.start()
    for cp in cps:
        cp.wait()


def tiles(x, wt):
    rows = math.prod(x.shape) // (128 * wt)
    return x.reshape(rows // 8, 8, wt, 128).transpose(0, 2, 1, 3).reshape(rows * wt, 128)


def untiles(x, wt, shape):
    rows = x.shape[0] // wt
    return x.reshape(rows // 8, wt, 8, 128).transpose(0, 2, 1, 3).reshape(shape)


def solution(mesh):
    any_spec = pl.BlockSpec(memory_space=pl.ANY)
    vmem_spec = pl.BlockSpec(memory_space=pltpu.VMEM)
    dma = pltpu.SemaphoreType.DMA

    def vmem(*shape, dtype=F32):
        return pltpu.VMEM(shape + (128,), dtype)

    def body(g_emb, g_qkv, g_o, g_w1, g_w2, g_bqkv, g_b1, g_dvec, m, v, w, lr, beta1, beta2, eps, step):
        grads = (g_emb, g_qkv, g_o, g_w1, g_w2)
        shapes = tuple(g.shape[1:] for g in grads)
        big = [tiles(g, t[2]) for g, t in zip(grads, TENSORS)]
        tail = jnp.concatenate([g_bqkv.reshape(-1), g_b1.reshape(-1), g_dvec.reshape(-1)])
        tail = jnp.pad(tail, (0, TAIL_ROWS * 128 - tail.shape[0])).reshape(TAIL_ROWS, 128)
        t = step.astype(F32)
        sc = jnp.stack([lr, beta1, 1.0 - beta1, beta2, 1.0 - beta2,
                        1.0 / (1.0 - beta1 ** t), 1.0 / (1.0 - beta2 ** t), eps])
        front = LOCPAD * 128
        state = [pltpu.with_memory_space_constraint(
            jnp.pad(a, (front, SROWS * 128 - front - SHARD)).reshape(SROWS, 128), pltpu.VMEM) for a in (m, v, w)]
        ag, *new = pl.pallas_call(
            comm_kernel,
            out_shape=(pltpu.VMEM((2, 2, 2, 2, 2, NR, 128), BF16),) + (pltpu.VMEM((LROWS, 128), F32),) * 3,
            in_specs=[pl.BlockSpec(memory_space=pltpu.SMEM)] + [any_spec] * 6 + [vmem_spec] * 3,
            out_specs=(vmem_spec,) * 4,
            scratch_shapes=[vmem(SL, *[2] * (NST - 1 - st), n) for n in PARTS for st in range(NST)] + [
                vmem(2, 2, 2, 2, NR), vmem(S0, 2, 2, 2, 2, CH),
                vmem(3, FROWS), vmem(3, FROWS), vmem(3, HALO + 16), vmem(3, HALO + 16),
                vmem(NR + 2 * HALO), vmem(HALO), vmem(HALO + 16), vmem(NR + 2 * HALO),
                dma((S0,)), dma((S0,)), dma((S0,))] + [dma((3, NST, SL)) for _ in range(6)] + [
                dma((4,)), dma((4,)),
            ],
            compiler_params=pltpu.CompilerParams(has_side_effects=True, collective_id=0, vmem_limit_bytes=36 * 2 ** 20),
            name="reduce_adam_gather",
        )(sc, *big, tail, *state)
        outs = pl.pallas_call(
            unpack_kernel,
            out_shape=tuple(jax.ShapeDtypeStruct((b - a, 128), BF16) for a, b, _ in TENSORS)
            + (jax.ShapeDtypeStruct((TAIL_ROWS, 128), BF16),) + (jax.ShapeDtypeStruct((SHARD,), F32),) * 3,
            in_specs=[vmem_spec] * 4,
            out_specs=(any_spec,) * 9,
            scratch_shapes=[dma((DEV + 11,))],
            compiler_params=pltpu.CompilerParams(vmem_limit_bytes=2 ** 20),
            name="unpack",
        )(ag, *[a.reshape(-1)[:SHARD] for a in new])
        wb = [untiles(o, tt[2], s) for o, tt, s in zip(outs[:5], TENSORS, shapes)]
        flat = outs[5].reshape(-1)
        n1, n2 = g_bqkv.size, g_b1.size
        wb += [flat[:n1].reshape(g_bqkv.shape[1:]), flat[n1:n1 + n2].reshape(g_b1.shape[1:]),
               flat[n1 + n2:n1 + n2 + g_dvec.size].reshape(g_dvec.shape[1:])]
        return tuple(outs[6:]) + tuple(wb)

    g3 = P(AXES, None, None)
    g4 = P(AXES, None, None, None)
    flat = P(AXES)
    rep = P()
    in_specs = (g3, g4, g4, g4, g4, g3, g3, g4, flat, flat, flat, rep, rep, rep, rep, rep)
    out_specs = (flat, flat, flat, rep, rep, rep, rep, rep, rep, rep, rep)
    return jax.shard_map(body, mesh=mesh, in_specs=in_specs, out_specs=out_specs, check_vma=False)
```

```python
import functools
import math

import jax
import jax.numpy as jnp
from jax import lax
from jax.experimental import pallas as pl
from jax.experimental.pallas import tpu as pltpu
from jax.sharding import PartitionSpec as P

AXES = ("outer", "inner")
MESH = pl.DeviceIdType.MESH
F32 = jnp.float32
BF16 = jnp.bfloat16

DEV = 32
SHARD = 270616
ROWS16 = 33827
TENSORS = ((0, 24576, 6), (24576, 38400, 18), (38400, 43008, 6), (43008, 55296, 16), (55296, 67584, 6))
TAIL0 = 67584
TAIL_ROWS = 80
LAST_ROW = 67654
NR = 2128
K = 19
PARTS = (40, 40, 16, 16)
CH = sum(PARTS)
SL = 4
S0 = 5
AHEAD = 2
HALO = 160
LOCPAD = 24
LROWS = 2120
FROWS = 2464
SROWS = 2176


def win_start(r):
    if isinstance(r, int):
        return (r * ROWS16) // 256 * 16
    return lax.div(r * ROWS16, 256) * 16


def rows_of(r):
    lo, hi = win_start(r), win_start(r) + NR
    segs = []
    for i, (a, b, _) in enumerate(TENSORS + ((TAIL0, TAIL0 + TAIL_ROWS, 1),)):
        s, e = max(lo, a), min(hi, b)
        if s < e:
            segs.append((i, s - a, s - lo, e - s))
    return segs


def halo_rows(n):
    s = win_start(n)
    for a, b, wt in TENSORS + ((TAIL0, TAIL0 + TAIL_ROWS, 1),):
        if a <= s < b:
            first = a + (s - a) // (8 * wt) * 8 * wt
            end = first + 8 * wt
    return s + 16 - first // 16 * 16, max(16, -(-end // 16) * 16 - s) if first < s else 16


def al(i, n, a=8):
    return pl.ds(pl.multiple_of(i, a), n)


def bits(w, n):
    out = []
    for _ in range(n):
        out.append(lax.rem(w, 2))
        w = lax.div(w, 2)
    return tuple(out[::-1])


def loop_add(dst, src, lead, n):
    def one(w, _):
        d, s = dst(w), src(w)
        for o in range(0, n, 8):
            d[pl.ds(o, 8), :] = d[pl.ds(o, 8), :] + s[pl.ds(o, 8), :]
        return 0

    lax.fori_loop(0, lead, one, 0)


def adam(g, m, v, w, sc):
    lr, b1, c1, b2, c2, i1, i2, eps = sc
    m2 = b1 * m + c1 * g
    v2 = b2 * v + c2 * (g * g)
    w2 = w - lr * (m2 * i1) / (jnp.sqrt(v2 * i2) + eps)
    return m2, v2, w2


H, L, Y, X = range(4)
IN, MID, OUT = range(4, 7)
LINE = (IN, MID, OUT)
ORDERS = ((X, Y) + LINE, (Y, X) + LINE, LINE + (X, Y), LINE + (Y, X))
COLOURS = range(len(ORDERS))
STARTS = tuple(sum(PARTS[:k]) for k in COLOURS)
NST = len(ORDERS[0])
PIECES = [(k, st, p) for k in COLOURS for st in range(NST) for p in range(2 if ORDERS[k][st] == IN else 1)]


def free_axes(k, st, p):
    o = ORDERS[k]
    kind = o[st]
    free = [ax for ax in (Y, X) if o.index(ax) > st]
    if kind in (Y, X):
        free += [H, L] * (o.index(IN) > st)
    elif kind == MID or kind == IN and p == 1:
        free.append(L)
    return sorted(free)


def comm_kernel(sc_ref, e_ref, q_ref, o_ref, w1_ref, w2_ref, t_ref, m_ref, v_ref, w_ref, ag, m_out, v_out, w_out, *scratch):
    bufs, scratch = dict(zip(PIECES, scratch)), scratch[len(PIECES):]
    (S, R0, F, TIL, HP, HN, GT, GP, GN, FG,
     ld, s0s, s0r, rss, rsr, ags, agr, fws, fwr, ows, owr, hs, hr) = scratch
    z = lax.axis_index(AXES[0])
    inner = lax.axis_index(AXES[1])
    h, l, y, x, c = bits(z, 2) + bits(inner, 3)
    me = (h, l, y, x)
    r = z * 8 + inner
    g_refs = (e_ref, q_ref, o_ref, w1_ref, w2_ref, t_ref)
    sc = [sc_ref[i] for i in range(8)]
    state = (m_ref, v_ref, w_ref)

    end = h == l
    middle = h != l

    def flip(*axes):
        p = [1 - b if i in axes else b for i, b in enumerate(me)]
        return p[H] * 2 + p[L], p[Y] * 4 + p[X] * 2 + c

    PEER = {X: flip(X), Y: flip(Y), IN: flip(L), OUT: flip(L), MID: flip(H, L)}
    CORE = (z, inner + 1 - 2 * c)

    def device(i):
        i = lax.rem(i, DEV)
        return lax.div(i, 8), lax.rem(i, 8)

    NXT, PRV = device(r + 1), device(r + DEV - 1)

    def remote(src, dst, ss, rs, dev):
        return pltpu.make_async_remote_copy(src_ref=src, dst_ref=dst, send_sem=ss, recv_sem=rs,
                                            device_id=dev, device_id_type=MESH)

    def window_copies(w, q, make):
        segs = rows_of(w)
        off = q * CH
        if len(segs) == 1:
            i, a, _, _ = segs[0]
            make(g_refs[i].at[al(a + off, CH)], 0, CH)
            return
        for n, (i, a, b, size) in enumerate(segs):
            first, last = -(-b // CH), (b + size) // CH

            @pl.when(jnp.logical_and(q >= first, q < last))
            def _(i=i, a=a, b=b):
                make(g_refs[i].at[al(jnp.maximum(a + off - b, 0), CH)], 0, CH)

            if n + 1 < len(segs) and (b + size) % CH:
                edge, head = (b + size) // CH, (b + size) % CH
                j, a2, _, _ = segs[n + 1]

                @pl.when(q == edge)
                def _(i=i, a=a, size=size, head=head, j=j, a2=a2):
                    make(g_refs[i].at[pl.ds(a + size - head, head)], 0, head)
                    make(g_refs[j].at[pl.ds(a2, CH - head)], head, CH - head)

    def start0(q):
        slot = lax.rem(q, S0)
        for par in range(2):

            @pl.when(c == par)
            def _(par=par):
                for k in range(16):
                    idx = tuple(k >> i & 1 for i in (3, 2, 1, 0))

                    def send(src, o, n, idx=idx):
                        remote(src, R0.at[(slot,) + idx + (pl.ds(o, n),)], s0s.at[slot], s0r.at[slot], CORE).start()

                    def load(src, o, n, idx=idx):
                        pltpu.make_async_copy(src, S.at[idx + (al(q * CH + o, n),)], ld.at[slot]).start()

                    window_copies(2 * k + 1 - par, q, send)
                    window_copies(2 * k + par, q, load)

    def wait0(q):
        slot = lax.rem(q, S0)
        rows = S.at[:, :, :, :, al(q * CH, CH)]
        pltpu.make_async_copy(rows, rows, ld.at[slot]).wait()
        remote(R0.at[slot], R0.at[slot], s0s.at[slot], s0r.at[slot], CORE).wait()

    every = slice(None)

    def part(k, q):
        return al(q * CH + STARTS[k], PARTS[k])

    def piece(k, st, p):
        kind = ORDERS[k][st]
        away, home = list(me), list(me)
        for ax in free_axes(k, st, p):
            away[ax] = home[ax] = every
        if kind in (Y, X):
            away[kind] = 1 - me[kind]
            return away, home, None, None
        if kind == MID:
            away[H] = 1 - h
            return away, home, middle, middle
        if kind == OUT:
            away[L] = 1 - l
            return away, home, middle, end
        if p == 0:
            away[L] = 1 - l
        else:
            away[H] = home[H] = 1 - h
        return away, home, end, middle

    def by(role, body):
        if role is None:
            body()
        else:
            pl.when(role)(body)

    def sem(kp):
        return PIECES.index(kp)

    def rs_copy(kp, q):
        s, i = lax.rem(q, SL), sem(kp)
        away = piece(*kp)[0]
        return remote(S.at[tuple(away) + (part(kp[0], q),)], bufs[kp].at[s], rss.at[i, s], rsr.at[i, s],
                      PEER[ORDERS[kp[0]][kp[1]]])

    def ag_copy(kp, q, recv):
        s, i = lax.rem(q, SL), sem(kp)
        idx = piece(*kp)[0 if recv else 1]
        ref = ag.at[tuple(idx) + (c, part(kp[0], q))]
        return remote(ref, ref, ags.at[i, s], agr.at[i, s], PEER[ORDERS[kp[0]][kp[1]]])

    def fw_copy(kp, q, core):
        s, i = lax.rem(q, SL), sem(kp)
        ref = ag.at[tuple(piece(*kp)[0]) + (core, part(kp[0], q))]
        return remote(ref, ref, fws.at[i, s], fwr.at[i, s], CORE)

    def own_copy(q, core):
        s = lax.rem(q, SL)
        ref = ag.at[me + (core, al(q * CH, CH))]
        return remote(ref, ref, ows.at[s], owr.at[s], CORE)

    def start(cp, q):
        @pl.when(q >= SL)
        def _():
            cp.wait_send()

        cp.start()

    def at(st, k=None):
        return [kp for kp in PIECES if kp[1] == st and k in (None, kp[0])]

    def rs_start(st, q, k=None):
        for kp in at(st, k):
            by(piece(*kp)[2], lambda kp=kp: start(rs_copy(kp, q), q))

    def ag_start(st, q, k=None):
        for kp in at(st, k):
            by(piece(*kp)[3], lambda kp=kp: start(ag_copy(kp, q, False), q))

    def rs_finish(st, q, k):
        for kp in at(st, k):
            _, home, _, gets = piece(*kp)
            free = free_axes(*kp)

            def dst(w, home=home, free=free):
                to = list(home)
                for ax, bit in zip(free, bits(w, len(free))):
                    to[ax] = bit
                return S.at[tuple(to) + (part(k, q),)]

            def src(w, kp=kp, free=free):
                return bufs[kp].at[(lax.rem(q, SL),) + bits(w, len(free))]

            def body(kp=kp, dst=dst, src=src, free=free):
                rs_copy(kp, q).wait_recv()
                loop_add(dst, src, 2 ** len(free), PARTS[k])

            by(gets, body)

    def ag_finish(st, q, k):
        for kp in at(st, k):
            by(piece(*kp)[2], lambda kp=kp: ag_copy(kp, q, True).wait_recv())

    def fw_start(st, q, k):
        for kp in at(st, k):
            by(piece(*kp)[2], lambda kp=kp: start(fw_copy(kp, q, c), q))

    def fw_finish(st, q, k):
        for kp in at(st, k):
            by(piece(*kp)[2], lambda kp=kp: fw_copy(kp, q, 1 - c).wait_recv())

    sr, srn = win_start(r), win_start(r + 1)
    delta = lax.rem(r * 24, 128)
    drow = lax.div(r * ROWS16, 16) - sr
    edge_n = lax.rem((r + 1) * 24, 128) + 128 * (lax.div((r + 1) * ROWS16, 16) - srn)
    nb = HALO + srn - sr
    lane = lax.broadcasted_iota(jnp.int32, (8, 128), 1)
    sub = lax.broadcasted_iota(jnp.int32, (8, 128), 0)

    def halo_up(n):
        size, _ = halo_rows(n)
        o = pl.ds(HALO + 16 - size, size)
        return remote(F.at[:, al(nb + 16 - size, size)], HP.at[:, o], hs.at[0], hr.at[0], NXT)

    def halo_down(n):
        _, size = halo_rows(n)
        return remote(F.at[:, pl.ds(HALO, size)], HN.at[:, pl.ds(0, size)], hs.at[1], hr.at[1], PRV)

    def halos(sent, received):
        for n in range(DEV):
            @pl.when(r == n)
            def _(n=n):
                for cp in [halo_up(n + 1)] * (n + 1 < DEV) + [halo_down(n)] * (n > 0):
                    sent(cp)
                if received is not None:
                    for cp in [halo_down(n + 1)] * (n + 1 < DEV) + [halo_up(n)] * (n > 0):
                        received(cp)

    def shift(ref, at, other, by, keep):
        return pltpu.roll(jnp.where(keep, ref[pl.ds(at, 8), :], ref[pl.ds(at + other, 8), :]), by, 1)

    def prepare1(lo, hi):
        keep = lane < 128 - delta

        def one(i, _):
            for j in range(4):
                at = i * 32 + j * 8
                for k in range(3):
                    F[k, al(HALO + at, 8), :] = shift(state[k], LOCPAD + at - drow, -1, delta, keep)
            return 0

        lax.fori_loop(lo, hi, one, 0)

    def blocks(first, last, body):
        for a, b, wt in TENSORS + ((TAIL0, TAIL0 + TAIL_ROWS, 1),):
            lo = lax.div(jnp.maximum(first - a, 0), 8 * wt)
            hi = lax.div(jnp.maximum(jnp.minimum(last, b) - a, 0) + 8 * wt - 1, 8 * wt)

            def one(i, _, a=a, wt=wt):
                body(a + i * 8 * wt, wt)
                return 0

            lax.fori_loop(lo, hi, one, 0)

    def prepare2():
        halos(lambda cp: cp.wait_send(), lambda cp: cp.wait_recv())
        for k in range(3):
            for i in range(0, 16, 8):
                idx = (sub + i) * 128 + lane
                o = pl.ds(HALO + i, 8)
                F[k, o, :] = jnp.where(idx < drow * 128 + delta, HP[k, o, :], F[k, o, :])
                o = al(nb + i, 8)
                F[k, o, :] = jnp.where(idx >= edge_n, HN[k, pl.ds(i, 8), :], F[k, o, :])

        def one(i, _):
            for k in range(3):
                F[k, al(i * 16, 16), :] = HP[k, al(i * 16, 16), :]
                F[k, al(nb + 16 + i * 16, 16), :] = HN[k, al(16 + i * 16, 16), :]
            return 0

        lax.fori_loop(0, HALO // 16, one, 0)

    def prepare3(ks):
        def permute(row, wt):
            at = row - sr + HALO
            for j in range(wt):
                for k in ks:
                    TIL[k, al(at + 8 * j, 8), :] = (
                        F[k, pl.ds(at + j, 8, stride=wt), :] if wt > 1 else F[k, al(at, 8), :])

        blocks(sr, sr + NR, permute)

    def ghalo_copies():
        return [remote(GT.at[al(nb - HALO, HALO)], GP, hs.at[2], hr.at[2], NXT),
                remote(GT.at[pl.ds(HALO, HALO + 16)], GN, hs.at[3], hr.at[3], PRV)]

    def finish2():
        for cp in ghalo_copies():
            cp.wait()

        def put(i, _):
            GT[al(i * 16, 16), :] = GP[al(i * 16, 16), :]
            GT[al(HALO + NR + i * 16, 16), :] = GN[al(HALO + NR - nb + i * 16, 16), :]
            return 0

        lax.fori_loop(0, HALO // 16, put, 0)

        def permute(row, wt):
            at = row - sr + HALO
            for j in range(wt):
                v = GT[al(at + 8 * j, 8), :]
                if wt > 1:
                    FG[pl.ds(at + j, 8, stride=wt), :] = v
                else:
                    FG[al(at, 8), :] = v

        blocks(sr, srn + 16, permute)

    def finish3(lo, hi):
        back = lax.rem(128 - delta, 128)

        def one(i, _):
            for j in range(5):
                at = i * 40 + j * 8
                g = shift(FG, HALO + drow + at, 1, back, lane >= delta)
                new = adam(g, *[ref[al(LOCPAD + at, 8), :] for ref in state], sc)
                for ref, val in zip((m_out, v_out, w_out), new):
                    ref[al(at, 8), :] = val
            return 0

        lax.fori_loop(lo, hi, one, 0)

    barrier = pltpu.get_barrier_semaphore()
    friends = [PEER[X], PEER[Y], PEER[IN], PEER[MID], CORE, NXT, PRV]
    for dev in friends:
        pl.semaphore_signal(barrier, inc=1, device_id=dev, device_id_type=MESH)
    pl.semaphore_wait(barrier, len(friends))
    for q in range(AHEAD):
        start0(q)
    turns, edge_turns = (NR + 16) // 32, (HALO + 32) // 32
    prepare1(0, edge_turns)
    prepare1(turns - edge_turns, turns)
    halos(lambda cp: cp.start(), None)

    def step(s, _):
        def at_stage(n, body):
            q = s - n

            @pl.when(jnp.logical_and(q >= 0, q < K))
            def _():
                body(q)

        def first(q):
            wait0(q)

            @pl.when(q + AHEAD < K)
            def _():
                start0(q + AHEAD)

            slot = lax.rem(q, S0)
            loop_add(lambda w: S.at[bits(w, 4) + (al(q * CH, CH),)], lambda w: R0.at[(slot,) + bits(w, 4)], 16, CH)
            rs_start(0, q)

        at_stage(0, first)

        for st in range(1, NST):
            def middle(q, st=st):
                for k in COLOURS:
                    rs_finish(st - 1, q, k)
                    rs_start(st, q, k)

            at_stage(st, middle)

        def update(q):
            for k in COLOURS:
                rs_finish(NST - 1, q, k)

            def one(i, _):
                o = al(q * CH + i * 16, 16)
                oh = al(HALO + q * CH + i * 16, 16)
                g = S[me + (o,)] * (1.0 / DEV)
                GT[oh, :] = g
                _, _, w2 = adam(g, TIL[0, oh, :], TIL[1, oh, :], TIL[2, oh, :], sc)
                ag[me + (c, o)] = w2.astype(BF16)
                return 0

            lax.fori_loop(0, CH // 16, one, 0)
            ag_start(NST - 1, q)
            start(own_copy(q, c), q)

        at_stage(NST, update)

        for st in range(NST):
            def gather(q, st=NST - 1 - st):
                if st == NST - 1:
                    own_copy(q, 1 - c).wait_recv()
                for k in COLOURS:
                    ag_finish(st, q, k)
                    if st:
                        ag_start(st - 1, q, k)
                    if st + 1 < NST:
                        fw_finish(st + 1, q, k)
                    fw_start(st, q, k)

            at_stage(NST + 1 + st, gather)

        def last(q):
            for k in COLOURS:
                fw_finish(0, q, k)

        at_stage(2 * NST + 1, last)

        def send_halos():
            for cp in ghalo_copies():
                cp.start()

        done, outer = K + NST - 1, LROWS // 40
        extra = {
            0: lambda: prepare1(edge_turns, turns // 2),
            1: lambda: prepare1(turns // 2, turns - edge_turns),
            2: lambda: (prepare2(), prepare3((0,))),
            3: lambda: prepare3((1, 2)),
            done: send_halos,
            done + 1: finish2,
        }
        cuts = [outer * i // NST for i in range(NST + 1)]
        for i in range(NST):
            extra[done + 2 + i] = lambda i=i: finish3(cuts[i], cuts[i + 1])
        for n, f in extra.items():
            @pl.when(s == n)
            def _(f=f):
                f()

        return 0

    lax.fori_loop(0, K + 2 * NST + 1, step, 0)

    def drain(i, _):
        q = K - SL + i
        own_copy(q, c).wait_send()
        for kp in PIECES:
            _, _, away, home = piece(*kp)
            by(away, lambda kp=kp: rs_copy(kp, q).wait_send())
            by(away, lambda kp=kp: fw_copy(kp, q, c).wait_send())
            by(home, lambda kp=kp: ag_copy(kp, q, False).wait_send())
        return 0

    lax.fori_loop(0, SL, drain, 0)


def unpack_kernel(ag, m_new, v_new, w_new, e_out, q_out, o_out, w1_out, w2_out, t_out, m_out, v_out, w_out, sem):
    outs = (e_out, q_out, o_out, w1_out, w2_out, t_out)
    cps = [pltpu.make_async_copy(src, dst, sem.at[DEV + 8 + k])
           for k, (src, dst) in enumerate(((m_new, m_out), (v_new, v_out), (w_new, w_out)))]
    for r in range(DEV):
        end = min(win_start(r + 1), TAIL0 + TAIL_ROWS) - win_start(r) if r + 1 < DEV else NR
        for i, a, b, size in rows_of(r):
            size = min(size, end - b)
            if size > 0:
                src = ag.at[tuple(r >> j & 1 for j in (4, 3, 2, 1, 0)) + (pl.ds(b, size),)]
                cps.append(pltpu.make_async_copy(src, outs[i].at[pl.ds(a, size)], sem.at[len(cps) - 3]))
    for cp in cps:
        cp.start()
    for cp in cps:
        cp.wait()


def tiles(x, wt):
    rows = math.prod(x.shape) // (128 * wt)
    return x.reshape(rows // 8, 8, wt, 128).transpose(0, 2, 1, 3).reshape(rows * wt, 128)


def untiles(x, wt, shape):
    rows = x.shape[0] // wt
    return x.reshape(rows // 8, wt, 8, 128).transpose(0, 2, 1, 3).reshape(shape)


def solution(mesh):
    any_spec = pl.BlockSpec(memory_space=pl.ANY)
    vmem_spec = pl.BlockSpec(memory_space=pltpu.VMEM)
    dma = pltpu.SemaphoreType.DMA

    def vmem(*shape, dtype=F32):
        return pltpu.VMEM(shape + (128,), dtype)

    def body(g_emb, g_qkv, g_o, g_w1, g_w2, g_bqkv, g_b1, g_dvec, m, v, w, lr, beta1, beta2, eps, step):
        grads = (g_emb, g_qkv, g_o, g_w1, g_w2)
        shapes = tuple(g.shape[1:] for g in grads)
        big = [tiles(g, t[2]) for g, t in zip(grads, TENSORS)]
        tail = jnp.concatenate([g_bqkv.reshape(-1), g_b1.reshape(-1), g_dvec.reshape(-1)])
        tail = jnp.pad(tail, (0, TAIL_ROWS * 128 - tail.shape[0])).reshape(TAIL_ROWS, 128)
        t = step.astype(F32)
        sc = jnp.stack([lr, beta1, 1.0 - beta1, beta2, 1.0 - beta2,
                        1.0 / (1.0 - beta1 ** t), 1.0 / (1.0 - beta2 ** t), eps])
        front = LOCPAD * 128
        state = [pltpu.with_memory_space_constraint(
            jnp.pad(a, (front, SROWS * 128 - front - SHARD)).reshape(SROWS, 128), pltpu.VMEM) for a in (m, v, w)]
        ag, *new = pl.pallas_call(
            comm_kernel,
            out_shape=(pltpu.VMEM((2, 2, 2, 2, 2, NR, 128), BF16),) + (pltpu.VMEM((LROWS, 128), F32),) * 3,
            in_specs=[pl.BlockSpec(memory_space=pltpu.SMEM)] + [any_spec] * 6 + [vmem_spec] * 3,
            out_specs=(vmem_spec,) * 4,
            scratch_shapes=[vmem(SL, *[2] * len(free_axes(*kp)), PARTS[kp[0]]) for kp in PIECES] + [
                vmem(2, 2, 2, 2, NR), vmem(S0, 2, 2, 2, 2, CH),
                vmem(3, FROWS), vmem(3, FROWS), vmem(3, HALO + 16), vmem(3, HALO + 16),
                vmem(NR + 2 * HALO), vmem(HALO), vmem(HALO + 16), vmem(NR + 2 * HALO),
                dma((S0,)), dma((S0,)), dma((S0,))] + [dma((len(PIECES), SL)) for _ in range(6)] + [
                dma((SL,)), dma((SL,)), dma((4,)), dma((4,)),
            ],
            compiler_params=pltpu.CompilerParams(has_side_effects=True, collective_id=0, vmem_limit_bytes=38 * 2 ** 20),
            name="reduce_adam_gather",
        )(sc, *big, tail, *state)
        outs = pl.pallas_call(
            unpack_kernel,
            out_shape=tuple(jax.ShapeDtypeStruct((b - a, 128), BF16) for a, b, _ in TENSORS)
            + (jax.ShapeDtypeStruct((TAIL_ROWS, 128), BF16),) + (jax.ShapeDtypeStruct((SHARD,), F32),) * 3,
            in_specs=[vmem_spec] * 4,
            out_specs=(any_spec,) * 9,
            scratch_shapes=[dma((DEV + 11,))],
            compiler_params=pltpu.CompilerParams(vmem_limit_bytes=2 ** 20),
            name="unpack",
        )(ag, *[a.reshape(-1)[:SHARD] for a in new])
        wb = [untiles(o, tt[2], s) for o, tt, s in zip(outs[:5], TENSORS, shapes)]
        flat = outs[5].reshape(-1)
        n1, n2 = g_bqkv.size, g_b1.size
        wb += [flat[:n1].reshape(g_bqkv.shape[1:]), flat[n1:n1 + n2].reshape(g_b1.shape[1:]),
               flat[n1 + n2:n1 + n2 + g_dvec.size].reshape(g_dvec.shape[1:])]
        return tuple(outs[6:]) + tuple(wb)

    g3 = P(AXES, None, None)
    g4 = P(AXES, None, None, None)
    flat = P(AXES)
    rep = P()
    in_specs = (g3, g4, g4, g4, g4, g3, g3, g4, flat, flat, flat, rep, rep, rep, rep, rep)
    out_specs = (flat, flat, flat, rep, rep, rep, rep, rep, rep, rep, rep)
    return jax.shard_map(body, mesh=mesh, in_specs=in_specs, out_specs=out_specs, check_vma=False)
```

```python
import functools
import math

import jax
import jax.numpy as jnp
from jax import lax
from jax.experimental import pallas as pl
from jax.experimental.pallas import tpu as pltpu
from jax.sharding import PartitionSpec as P

AXES = ("outer", "inner")
MESH = pl.DeviceIdType.MESH
F32 = jnp.float32
BF16 = jnp.bfloat16

DEV = 32
SHARD = 270616
ROWS16 = 33827
TENSORS = ((0, 24576, 6), (24576, 38400, 18), (38400, 43008, 6), (43008, 55296, 16), (55296, 67584, 6))
TAIL0 = 67584
TAIL_ROWS = 80
LAST_ROW = 67654
NR = 2128
K = 19
PARTS = (40, 40, 16, 16)
CH = sum(PARTS)
SL = 4
S0 = 5
AHEAD = 2
HALO = 160
LOCPAD = 24
LROWS = 2120
FROWS = 2464
SROWS = 2176


def win_start(r):
    if isinstance(r, int):
        return (r * ROWS16) // 256 * 16
    return lax.div(r * ROWS16, 256) * 16


def rows_of(r):
    lo, hi = win_start(r), win_start(r) + NR
    segs = []
    for i, (a, b, _) in enumerate(TENSORS + ((TAIL0, TAIL0 + TAIL_ROWS, 1),)):
        s, e = max(lo, a), min(hi, b)
        if s < e:
            segs.append((i, s - a, s - lo, e - s))
    return segs


def halo_rows(n):
    s = win_start(n)
    for a, b, wt in TENSORS + ((TAIL0, TAIL0 + TAIL_ROWS, 1),):
        if a <= s < b:
            first = a + (s - a) // (8 * wt) * 8 * wt
            end = first + 8 * wt
    return s + 16 - first // 16 * 16, max(16, -(-end // 16) * 16 - s) if first < s else 16


def al(i, n, a=8):
    return pl.ds(pl.multiple_of(i, a), n)


def bits(w, n):
    out = []
    for _ in range(n):
        out.append(lax.rem(w, 2))
        w = lax.div(w, 2)
    return tuple(out[::-1])


def loop_add(dst, src, lead, n):
    def one(w, _):
        d, s = dst(w), src(w)
        for o in range(0, n, 8):
            d[pl.ds(o, 8), :] = d[pl.ds(o, 8), :] + s[pl.ds(o, 8), :]
        return 0

    lax.fori_loop(0, lead, one, 0)


def adam(g, m, v, w, sc):
    lr, b1, c1, b2, c2, i1, i2, eps = sc
    m2 = b1 * m + c1 * g
    v2 = b2 * v + c2 * (g * g)
    w2 = w - lr * (m2 * i1) / (jnp.sqrt(v2 * i2) + eps)
    return m2, v2, w2


H, L, Y, X = range(4)
IN, MID, OUT = range(4, 7)
LINE = (IN, MID, OUT)
ORDERS = ((X, Y) + LINE, (Y, X) + LINE, LINE + (X, Y), LINE + (Y, X))
COLOURS = range(len(ORDERS))
STARTS = tuple(sum(PARTS[:k]) for k in COLOURS)
NST = len(ORDERS[0])
PIECES = [(k, st, p) for k in COLOURS for st in range(NST) for p in range(2 if ORDERS[k][st] == IN else 1)]


def free_axes(k, st, p):
    o = ORDERS[k]
    kind = o[st]
    free = [ax for ax in (Y, X) if o.index(ax) > st]
    if kind in (Y, X):
        free += [H, L] * (o.index(IN) > st)
    elif kind == MID or kind == IN and p == 1:
        free.append(L)
    return sorted(free)


def comm_kernel(sc_ref, e_ref, q_ref, o_ref, w1_ref, w2_ref, t_ref, m_ref, v_ref, w_ref, ag, m_out, v_out, w_out, *scratch):
    bufs, scratch = dict(zip(PIECES, scratch)), scratch[len(PIECES):]
    (S, R0, F, TIL, HP, HN, GT, GP, GN, FG,
     ld, s0s, s0r, rss, rsr, ags, agr, fws, fwr, ows, owr, hs, hr) = scratch
    z = lax.axis_index(AXES[0])
    inner = lax.axis_index(AXES[1])
    h, l, y, x, c = bits(z, 2) + bits(inner, 3)
    me = (h, l, y, x)
    r = z * 8 + inner
    g_refs = (e_ref, q_ref, o_ref, w1_ref, w2_ref, t_ref)
    sc = [sc_ref[i] for i in range(8)]
    state = (m_ref, v_ref, w_ref)

    end = h == l
    middle = h != l

    def flip(*axes):
        p = [1 - b if i in axes else b for i, b in enumerate(me)]
        return p[H] * 2 + p[L], p[Y] * 4 + p[X] * 2 + c

    PEER = {X: flip(X), Y: flip(Y), IN: flip(L), OUT: flip(L), MID: flip(H, L)}
    CORE = (z, inner + 1 - 2 * c)

    def device(i):
        i = lax.rem(i, DEV)
        return lax.div(i, 8), lax.rem(i, 8)

    NXT, PRV = device(r + 1), device(r + DEV - 1)

    def remote(src, dst, ss, rs, dev):
        return pltpu.make_async_remote_copy(src_ref=src, dst_ref=dst, send_sem=ss, recv_sem=rs,
                                            device_id=dev, device_id_type=MESH)

    def window_copies(w, q, make):
        segs = rows_of(w)
        off = q * CH
        if len(segs) == 1:
            i, a, _, _ = segs[0]
            make(g_refs[i].at[al(a + off, CH)], 0, CH)
            return
        for n, (i, a, b, size) in enumerate(segs):
            first, last = -(-b // CH), (b + size) // CH

            @pl.when(jnp.logical_and(q >= first, q < last))
            def _(i=i, a=a, b=b):
                make(g_refs[i].at[al(jnp.maximum(a + off - b, 0), CH)], 0, CH)

            if n + 1 < len(segs) and (b + size) % CH:
                edge, head = (b + size) // CH, (b + size) % CH
                j, a2, _, _ = segs[n + 1]

                @pl.when(q == edge)
                def _(i=i, a=a, size=size, head=head, j=j, a2=a2):
                    make(g_refs[i].at[pl.ds(a + size - head, head)], 0, head)
                    make(g_refs[j].at[pl.ds(a2, CH - head)], head, CH - head)

    def start0(q):
        slot = lax.rem(q, S0)
        for par in range(2):

            @pl.when(c == par)
            def _(par=par):
                for k in range(16):
                    idx = tuple(k >> i & 1 for i in (3, 2, 1, 0))

                    def send(src, o, n, idx=idx):
                        remote(src, R0.at[(slot,) + idx + (pl.ds(o, n),)], s0s.at[slot], s0r.at[slot], CORE).start()

                    def load(src, o, n, idx=idx):
                        pltpu.make_async_copy(src, S.at[idx + (al(q * CH + o, n),)], ld.at[slot]).start()

                    window_copies(2 * k + 1 - par, q, send)
                    window_copies(2 * k + par, q, load)

    def wait0(q):
        slot = lax.rem(q, S0)
        rows = S.at[:, :, :, :, al(q * CH, CH)]
        pltpu.make_async_copy(rows, rows, ld.at[slot]).wait()
        remote(R0.at[slot], R0.at[slot], s0s.at[slot], s0r.at[slot], CORE).wait()

    every = slice(None)

    def part(k, q):
        return al(q * CH + STARTS[k], PARTS[k])

    def piece(k, st, p):
        kind = ORDERS[k][st]
        away, home = list(me), list(me)
        for ax in free_axes(k, st, p):
            away[ax] = home[ax] = every
        if kind in (Y, X):
            away[kind] = 1 - me[kind]
            return away, home, None, None
        if kind == MID:
            away[H] = 1 - h
            return away, home, middle, middle
        if kind == OUT:
            away[L] = 1 - l
            return away, home, middle, end
        if p == 0:
            away[L] = 1 - l
        else:
            away[H] = home[H] = 1 - h
        return away, home, end, middle

    def by(role, body):
        if role is None:
            body()
        else:
            pl.when(role)(body)

    def sem(kp):
        return PIECES.index(kp)

    def rs_copy(kp, q):
        s, i = lax.rem(q, SL), sem(kp)
        away = piece(*kp)[0]
        return remote(S.at[tuple(away) + (part(kp[0], q),)], bufs[kp].at[s], rss.at[i, s], rsr.at[i, s],
                      PEER[ORDERS[kp[0]][kp[1]]])

    def ag_copy(kp, q, recv):
        s, i = lax.rem(q, SL), sem(kp)
        idx = piece(*kp)[0 if recv else 1]
        ref = ag.at[tuple(idx) + (c, part(kp[0], q))]
        return remote(ref, ref, ags.at[i, s], agr.at[i, s], PEER[ORDERS[kp[0]][kp[1]]])

    def fw_copy(kp, q, core):
        s, i = lax.rem(q, SL), sem(kp)
        ref = ag.at[tuple(piece(*kp)[0]) + (core, part(kp[0], q))]
        return remote(ref, ref, fws.at[i, s], fwr.at[i, s], CORE)

    def own_copy(q, core):
        s = lax.rem(q, SL)
        ref = ag.at[me + (core, al(q * CH, CH))]
        return remote(ref, ref, ows.at[s], owr.at[s], CORE)

    def start(cp, q):
        @pl.when(q >= SL)
        def _():
            cp.wait_send()

        cp.start()

    def at(st, k=None):
        return [kp for kp in PIECES if kp[1] == st and k in (None, kp[0])]

    def rs_start(st, q, k=None):
        for kp in at(st, k):
            by(piece(*kp)[2], lambda kp=kp: start(rs_copy(kp, q), q))

    def ag_start(st, q, k=None):
        for kp in at(st, k):
            by(piece(*kp)[3], lambda kp=kp: start(ag_copy(kp, q, False), q))

    def rs_finish(st, q, k):
        for kp in at(st, k):
            _, home, _, gets = piece(*kp)
            free = free_axes(*kp)

            def dst(w, home=home, free=free):
                to = list(home)
                for ax, bit in zip(free, bits(w, len(free))):
                    to[ax] = bit
                return S.at[tuple(to) + (part(k, q),)]

            def src(w, kp=kp, free=free):
                return bufs[kp].at[(lax.rem(q, SL),) + bits(w, len(free))]

            def body(kp=kp, dst=dst, src=src, free=free):
                rs_copy(kp, q).wait_recv()
                loop_add(dst, src, 2 ** len(free), PARTS[k])

            by(gets, body)

    def ag_finish(st, q, k):
        for kp in at(st, k):
            by(piece(*kp)[2], lambda kp=kp: ag_copy(kp, q, True).wait_recv())

    def fw_start(st, q, k):
        for kp in at(st, k):
            by(piece(*kp)[2], lambda kp=kp: start(fw_copy(kp, q, c), q))

    def fw_finish(st, q, k):
        for kp in at(st, k):
            by(piece(*kp)[2], lambda kp=kp: fw_copy(kp, q, 1 - c).wait_recv())

    sr, srn = win_start(r), win_start(r + 1)
    delta = lax.rem(r * 24, 128)
    drow = lax.div(r * ROWS16, 16) - sr
    edge_n = lax.rem((r + 1) * 24, 128) + 128 * (lax.div((r + 1) * ROWS16, 16) - srn)
    nb = HALO + srn - sr
    lane = lax.broadcasted_iota(jnp.int32, (8, 128), 1)
    sub = lax.broadcasted_iota(jnp.int32, (8, 128), 0)

    def halo_up(n):
        size, _ = halo_rows(n)
        o = pl.ds(HALO + 16 - size, size)
        return remote(F.at[:, al(nb + 16 - size, size)], HP.at[:, o], hs.at[0], hr.at[0], NXT)

    def halo_down(n):
        _, size = halo_rows(n)
        return remote(F.at[:, pl.ds(HALO, size)], HN.at[:, pl.ds(0, size)], hs.at[1], hr.at[1], PRV)

    def halos(sent, received):
        for n in range(DEV):
            @pl.when(r == n)
            def _(n=n):
                for cp in [halo_up(n + 1)] * (n + 1 < DEV) + [halo_down(n)] * (n > 0):
                    sent(cp)
                if received is not None:
                    for cp in [halo_down(n + 1)] * (n + 1 < DEV) + [halo_up(n)] * (n > 0):
                        received(cp)

    def shift(ref, at, other, by, keep):
        return pltpu.roll(jnp.where(keep, ref[pl.ds(at, 8), :], ref[pl.ds(at + other, 8), :]), by, 1)

    def prepare1(lo, hi):
        keep = lane < 128 - delta

        def one(i, _):
            for j in range(4):
                at = i * 32 + j * 8
                for k in range(3):
                    F[k, al(HALO + at, 8), :] = shift(state[k], LOCPAD + at - drow, -1, delta, keep)
            return 0

        lax.fori_loop(lo, hi, one, 0)

    def blocks(first, last, body):
        for a, b, wt in TENSORS + ((TAIL0, TAIL0 + TAIL_ROWS, 1),):
            lo = lax.div(jnp.maximum(first - a, 0), 8 * wt)
            hi = lax.div(jnp.maximum(jnp.minimum(last, b) - a, 0) + 8 * wt - 1, 8 * wt)

            def one(i, _, a=a, wt=wt):
                body(a + i * 8 * wt, wt)
                return 0

            lax.fori_loop(lo, hi, one, 0)

    def prepare2():
        halos(lambda cp: cp.wait_send(), lambda cp: cp.wait_recv())
        for k in range(3):
            for i in range(0, 16, 8):
                idx = (sub + i) * 128 + lane
                o = pl.ds(HALO + i, 8)
                F[k, o, :] = jnp.where(idx < drow * 128 + delta, HP[k, o, :], F[k, o, :])
                o = al(nb + i, 8)
                F[k, o, :] = jnp.where(idx >= edge_n, HN[k, pl.ds(i, 8), :], F[k, o, :])

        def one(i, _):
            for k in range(3):
                F[k, al(i * 16, 16), :] = HP[k, al(i * 16, 16), :]
                F[k, al(nb + 16 + i * 16, 16), :] = HN[k, al(16 + i * 16, 16), :]
            return 0

        lax.fori_loop(0, HALO // 16, one, 0)

    def prepare3(ks):
        def permute(row, wt):
            at = row - sr + HALO
            for j in range(wt):
                for k in ks:
                    TIL[k, al(at + 8 * j, 8), :] = (
                        F[k, pl.ds(at + j, 8, stride=wt), :] if wt > 1 else F[k, al(at, 8), :])

        blocks(sr, sr + NR, permute)

    def ghalo_copies():
        return [remote(GT.at[al(nb - HALO, HALO)], GP, hs.at[2], hr.at[2], NXT),
                remote(GT.at[pl.ds(HALO, HALO + 16)], GN, hs.at[3], hr.at[3], PRV)]

    def finish2():
        for cp in ghalo_copies():
            cp.wait()

        def put(i, _):
            GT[al(i * 16, 16), :] = GP[al(i * 16, 16), :]
            GT[al(HALO + NR + i * 16, 16), :] = GN[al(HALO + NR - nb + i * 16, 16), :]
            return 0

        lax.fori_loop(0, HALO // 16, put, 0)

        def permute(row, wt):
            at = row - sr + HALO
            for j in range(wt):
                v = GT[al(at + 8 * j, 8), :]
                if wt > 1:
                    FG[pl.ds(at + j, 8, stride=wt), :] = v
                else:
                    FG[al(at, 8), :] = v

        blocks(sr, srn + 16, permute)

    def finish3(lo, hi):
        back = lax.rem(128 - delta, 128)

        def one(i, _):
            for j in range(5):
                at = i * 40 + j * 8
                g = shift(FG, HALO + drow + at, 1, back, lane >= delta)
                new = adam(g, *[ref[al(LOCPAD + at, 8), :] for ref in state], sc)
                for ref, val in zip((m_out, v_out, w_out), new):
                    ref[al(at, 8), :] = val
            return 0

        lax.fori_loop(lo, hi, one, 0)

    barrier = pltpu.get_barrier_semaphore()
    friends = [PEER[X], PEER[Y], PEER[IN], PEER[MID], CORE, NXT, PRV]
    for dev in friends:
        pl.semaphore_signal(barrier, inc=1, device_id=dev, device_id_type=MESH)
    pl.semaphore_wait(barrier, len(friends))
    for q in range(AHEAD):
        start0(q)
    turns, edge_turns = (NR + 16) // 32, (HALO + 32) // 32
    prepare1(0, edge_turns)
    prepare1(turns - edge_turns, turns)
    halos(lambda cp: cp.start(), None)

    def step(s, _):
        def at_stage(n, body):
            q = s - n

            @pl.when(jnp.logical_and(q >= 0, q < K))
            def _():
                body(q)

        def first(q):
            wait0(q)

            @pl.when(q + AHEAD < K)
            def _():
                start0(q + AHEAD)

            slot = lax.rem(q, S0)
            loop_add(lambda w: S.at[bits(w, 4) + (al(q * CH, CH),)], lambda w: R0.at[(slot,) + bits(w, 4)], 16, CH)
            rs_start(0, q)

        at_stage(0, first)

        for st in range(1, NST):
            def middle(q, st=st):
                for k in COLOURS:
                    rs_finish(st - 1, q, k)
                    rs_start(st, q, k)

            at_stage(st, middle)

        def update(q):
            for k in COLOURS:
                rs_finish(NST - 1, q, k)

            def one(i, _):
                o = al(q * CH + i * 16, 16)
                oh = al(HALO + q * CH + i * 16, 16)
                g = S[me + (o,)] * (1.0 / DEV)
                GT[oh, :] = g
                _, _, w2 = adam(g, TIL[0, oh, :], TIL[1, oh, :], TIL[2, oh, :], sc)
                ag[me + (c, o)] = w2.astype(BF16)
                return 0

            lax.fori_loop(0, CH // 16, one, 0)
            ag_start(NST - 1, q)
            start(own_copy(q, c), q)

        at_stage(NST, update)

        for st in range(NST):
            def gather(q, st=NST - 1 - st):
                if st == NST - 1:
                    own_copy(q, 1 - c).wait_recv()
                for k in COLOURS:
                    ag_finish(st, q, k)
                    if st:
                        ag_start(st - 1, q, k)
                    if st + 1 < NST:
                        fw_finish(st + 1, q, k)
                    fw_start(st, q, k)

            at_stage(NST + 1 + st, gather)

        def last(q):
            for k in COLOURS:
                fw_finish(0, q, k)

        at_stage(2 * NST + 1, last)

        def send_halos():
            for cp in ghalo_copies():
                cp.start()

        done, outer = K + NST - 1, LROWS // 40
        extra = {
            0: lambda: prepare1(edge_turns, turns // 2),
            1: lambda: prepare1(turns // 2, turns - edge_turns),
            2: lambda: (prepare2(), prepare3((0,))),
            3: lambda: prepare3((1, 2)),
            done: send_halos,
            done + 1: finish2,
        }
        cuts = [outer * i // NST for i in range(NST + 1)]
        for i in range(NST):
            extra[done + 2 + i] = lambda i=i: finish3(cuts[i], cuts[i + 1])
        for n, f in extra.items():
            @pl.when(s == n)
            def _(f=f):
                f()

        return 0

    lax.fori_loop(0, K + 2 * NST + 1, step, 0)

    def drain(i, _):
        q = K - SL + i
        own_copy(q, c).wait_send()
        for kp in PIECES:
            _, _, away, home = piece(*kp)
            by(away, lambda kp=kp: rs_copy(kp, q).wait_send())
            by(away, lambda kp=kp: fw_copy(kp, q, c).wait_send())
            by(home, lambda kp=kp: ag_copy(kp, q, False).wait_send())
        return 0

    lax.fori_loop(0, SL, drain, 0)


def unpack_kernel(ag, m_new, v_new, w_new, e_out, q_out, o_out, w1_out, w2_out, t_out, m_out, v_out, w_out, sem):
    outs = (e_out, q_out, o_out, w1_out, w2_out, t_out)
    cps = [pltpu.make_async_copy(src, dst, sem.at[DEV + 8 + k])
           for k, (src, dst) in enumerate(((m_new, m_out), (v_new, v_out), (w_new, w_out)))]
    for r in range(DEV):
        end = min(win_start(r + 1), TAIL0 + TAIL_ROWS) - win_start(r) if r + 1 < DEV else NR
        for i, a, b, size in rows_of(r):
            size = min(size, end - b)
            if size > 0:
                src = ag.at[tuple(r >> j & 1 for j in (4, 3, 2, 1, 0)) + (pl.ds(b, size),)]
                cps.append(pltpu.make_async_copy(src, outs[i].at[pl.ds(a, size)], sem.at[len(cps) - 3]))
    for cp in cps:
        cp.start()
    for cp in cps:
        cp.wait()


def tiles(x, wt):
    rows = math.prod(x.shape) // (128 * wt)
    return x.reshape(rows // 8, 8, wt, 128).transpose(0, 2, 1, 3).reshape(rows * wt, 128)


def untiles(x, wt, shape):
    rows = x.shape[0] // wt
    return x.reshape(rows // 8, wt, 8, 128).transpose(0, 2, 1, 3).reshape(shape)


def solution(mesh):
    any_spec = pl.BlockSpec(memory_space=pl.ANY)
    vmem_spec = pl.BlockSpec(memory_space=pltpu.VMEM)
    dma = pltpu.SemaphoreType.DMA

    def vmem(*shape, dtype=F32):
        return pltpu.VMEM(shape + (128,), dtype)

    def body(g_emb, g_qkv, g_o, g_w1, g_w2, g_bqkv, g_b1, g_dvec, m, v, w, lr, beta1, beta2, eps, step):
        grads = (g_emb, g_qkv, g_o, g_w1, g_w2)
        shapes = tuple(g.shape[1:] for g in grads)
        big = [tiles(g, t[2]) for g, t in zip(grads, TENSORS)]
        tail = jnp.concatenate([g.reshape(1, -1) for g in (g_bqkv, g_b1, g_dvec)], axis=1)
        tail = jnp.pad(tail, ((0, 0), (0, TAIL_ROWS * 128 - tail.shape[1]))).reshape(TAIL_ROWS, 128)
        t = step.astype(F32)
        sc = jnp.stack([lr, beta1, 1.0 - beta1, beta2, 1.0 - beta2,
                        1.0 / (1.0 - beta1 ** t), 1.0 / (1.0 - beta2 ** t), eps])
        front = LOCPAD * 128
        state = [pltpu.with_memory_space_constraint(
            jnp.pad(a, (front, SROWS * 128 - front - SHARD)).reshape(SROWS, 128), pltpu.VMEM) for a in (m, v, w)]
        ag, *new = pl.pallas_call(
            comm_kernel,
            out_shape=(pltpu.VMEM((2, 2, 2, 2, 2, NR, 128), BF16),) + (pltpu.VMEM((LROWS, 128), F32),) * 3,
            in_specs=[pl.BlockSpec(memory_space=pltpu.SMEM)] + [any_spec] * 6 + [vmem_spec] * 3,
            out_specs=(vmem_spec,) * 4,
            scratch_shapes=[vmem(SL, *[2] * len(free_axes(*kp)), PARTS[kp[0]]) for kp in PIECES] + [
                vmem(2, 2, 2, 2, NR), vmem(S0, 2, 2, 2, 2, CH),
                vmem(3, FROWS), vmem(3, FROWS), vmem(3, HALO + 16), vmem(3, HALO + 16),
                vmem(NR + 2 * HALO), vmem(HALO), vmem(HALO + 16), vmem(NR + 2 * HALO),
                dma((S0,)), dma((S0,)), dma((S0,))] + [dma((len(PIECES), SL)) for _ in range(6)] + [
                dma((SL,)), dma((SL,)), dma((4,)), dma((4,)),
            ],
            compiler_params=pltpu.CompilerParams(has_side_effects=True, collective_id=0, vmem_limit_bytes=38 * 2 ** 20),
            name="reduce_adam_gather",
        )(sc, *big, tail, *state)
        outs = pl.pallas_call(
            unpack_kernel,
            out_shape=tuple(jax.ShapeDtypeStruct((b - a, 128), BF16) for a, b, _ in TENSORS)
            + (jax.ShapeDtypeStruct((TAIL_ROWS, 128), BF16),) + (jax.ShapeDtypeStruct((SHARD,), F32),) * 3,
            in_specs=[vmem_spec] * 4,
            out_specs=(any_spec,) * 9,
            scratch_shapes=[dma((DEV + 11,))],
            compiler_params=pltpu.CompilerParams(vmem_limit_bytes=2 ** 20),
            name="unpack",
        )(ag, *[a.reshape(-1)[:SHARD] for a in new])
        wb = [untiles(o, tt[2], s) for o, tt, s in zip(outs[:5], TENSORS, shapes)]
        flat = outs[5].reshape(-1)
        n1, n2 = g_bqkv.size, g_b1.size
        wb += [flat[:n1].reshape(g_bqkv.shape[1:]), flat[n1:n1 + n2].reshape(g_b1.shape[1:]),
               flat[n1 + n2:n1 + n2 + g_dvec.size].reshape(g_dvec.shape[1:])]
        return tuple(outs[6:]) + tuple(wb)

    g3 = P(AXES, None, None)
    g4 = P(AXES, None, None, None)
    flat = P(AXES)
    rep = P()
    in_specs = (g3, g4, g4, g4, g4, g3, g3, g4, flat, flat, flat, rep, rep, rep, rep, rep)
    out_specs = (flat, flat, flat, rep, rep, rep, rep, rep, rep, rep, rep)
    return jax.shard_map(body, mesh=mesh, in_specs=in_specs, out_specs=out_specs, check_vma=False)
```
